32 devices in a mesh: dp: 2 (over x), sp: 4 (over z), uly: 4 (over y, core).
Axes of the slice: x: 2, y: 2, z: 4, core: 2. Of those that a mesh axis runs over, the one named last changes fastest.
Arguments:
- tokens: bfloat16 [2, 4608, 5120], P('dp', ('sp', 'uly')), parts along dimension 0
- rope_ang: float32 [4608, 64], P(('sp', 'uly'))
- t_emb: float32 [2, 6, 5120], P('dp'), parts along dimension 0
- block_mod: float32 [1, 6, 5120], replicated
- context: bfloat16 [2, 512, 5120], P('dp'), parts along dimension 0
- attn_wq: bfloat16 [5120, 5120], replicated
- attn_bq: bfloat16 [5120], replicated
- attn_wk: bfloat16 [5120, 5120], replicated
- attn_bk: bfloat16 [5120], replicated
- attn_wv: bfloat16 [5120, 5120], replicated
- attn_bv: bfloat16 [5120], replicated
- attn_gq: bfloat16 [5120], replicated
- attn_gk: bfloat16 [5120], replicated
- attn_wo: bfloat16 [5120, 5120], replicated
- attn_bo: bfloat16 [5120], replicated
- norm3_w: bfloat16 [5120], replicated
- norm3_b: bfloat16 [5120], replicated
- cross_wq: bfloat16 [5120, 5120], replicated
- cross_wk: bfloat16 [5120, 5120], replicated
- cross_wv: bfloat16 [5120, 5120], replicated
- cross_gq: bfloat16 [5120], replicated
- cross_gk: bfloat16 [5120], replicated
- cross_wo: bfloat16 [5120, 5120], replicated
- ffn_w1: bfloat16 [5120, 13824], replicated
- ffn_w2: bfloat16 [13824, 5120], replicated
Outputs:
- output: bfloat16 [2, 4608, 5120], P('dp', ('sp', 'uly')), parts along dimension 0
There are 2 independent parts. The reference program is written for one: setup_inputs(seed, part) draws one part's arguments, and reference() takes and returns one part's arrays. A program takes and returns all parts, laid end to end along the dimension named above; an argument that names none is the same for every part.
All inputs are finite; a program needn't handle non-finite values.
Results may differ from the reference program's by a relative error of at most 0.00568233.
Values are sent between devices in bfloat16 or wider.
A program may use at most 2.75 GiB of HBM per device.

```python
import jax
import jax.numpy as jnp
from jax import lax

BATCH = 1
FRAMES = 3
ROWS = 48
COLS = 32
D = 5120
HEADS = 40
HEAD = 128
FF = 13824
TEXT = 512
SEQ = FRAMES * ROWS * COLS
FRAME_TOK = ROWS * COLS
EPS = 1e-6


def rope_table(table_key):
    frame_gaps = jax.random.randint(table_key, (FRAMES,), 1, 7)
    t_pos = (jnp.cumsum(frame_gaps) - frame_gaps[0]).astype(jnp.float32)
    h_pos = jnp.arange(ROWS).astype(jnp.float32)
    w_pos = jnp.arange(COLS).astype(jnp.float32)
    freq_t = 1.0 / (10000.0 ** (jnp.arange(0, 44, 2).astype(jnp.float32) / 44.0))
    freq_s = 1.0 / (10000.0 ** (jnp.arange(0, 42, 2).astype(jnp.float32) / 42.0))
    ang_t = jnp.broadcast_to((t_pos[:, None] * freq_t)[:, None, None, :], (FRAMES, ROWS, COLS, 22))
    ang_h = jnp.broadcast_to((h_pos[:, None] * freq_s)[None, :, None, :], (FRAMES, ROWS, COLS, 21))
    ang_w = jnp.broadcast_to((w_pos[:, None] * freq_s)[None, None, :, :], (FRAMES, ROWS, COLS, 21))
    return jnp.concatenate([ang_t, ang_h, ang_w], axis=-1).reshape(SEQ, 64)


def setup_inputs(seed: int = 0, part: int = 0) -> dict:
    root_key = jax.random.key(seed)
    part_keys = jax.random.split(jax.random.fold_in(root_key, part), 3)
    shared = jax.random.split(root_key, 24)

    def normal(sub_key, shape, scale):
        return jax.random.normal(sub_key, shape, jnp.float32) * scale

    scale_d = D ** -0.5
    scale_ff = FF ** -0.5
    return {
        'tokens': normal(part_keys[0], (BATCH, SEQ, D), 1.0).astype(jnp.bfloat16),
        'rope_ang': rope_table(shared[0]),
        't_emb': normal(part_keys[1], (BATCH, 6, D), 0.3),
        'block_mod': normal(shared[1], (1, 6, D), 0.3),
        'context': normal(part_keys[2], (BATCH, TEXT, D), 1.0).astype(jnp.bfloat16),
        'attn_wq': normal(shared[2], (D, D), scale_d).astype(jnp.bfloat16),
        'attn_bq': normal(shared[3], (D,), 0.5).astype(jnp.bfloat16),
        'attn_wk': normal(shared[4], (D, D), scale_d).astype(jnp.bfloat16),
        'attn_bk': normal(shared[5], (D,), 0.5).astype(jnp.bfloat16),
        'attn_wv': normal(shared[6], (D, D), scale_d).astype(jnp.bfloat16),
        'attn_bv': normal(shared[7], (D,), 0.5).astype(jnp.bfloat16),
        'attn_gq': (1.7 + normal(shared[8], (D,), 0.4)).astype(jnp.bfloat16),
        'attn_gk': (1.7 + normal(shared[9], (D,), 0.4)).astype(jnp.bfloat16),
        'attn_wo': normal(shared[10], (D, D), scale_d).astype(jnp.bfloat16),
        'attn_bo': normal(shared[11], (D,), 0.5).astype(jnp.bfloat16),
        'norm3_w': (1.0 + normal(shared[12], (D,), 0.3)).astype(jnp.bfloat16),
        'norm3_b': normal(shared[13], (D,), 0.5).astype(jnp.bfloat16),
        'cross_wq': normal(shared[14], (D, D), scale_d).astype(jnp.bfloat16),
        'cross_wk': normal(shared[15], (D, D), scale_d).astype(jnp.bfloat16),
        'cross_wv': normal(shared[16], (D, D), scale_d).astype(jnp.bfloat16),
        'cross_gq': (1.4 + normal(shared[17], (D,), 0.3)).astype(jnp.bfloat16),
        'cross_gk': (1.4 + normal(shared[18], (D,), 0.3)).astype(jnp.bfloat16),
        'cross_wo': normal(shared[19], (D, D), scale_d).astype(jnp.bfloat16),
        'ffn_w1': normal(shared[20], (D, FF), scale_d).astype(jnp.bfloat16),
        'ffn_w2': normal(shared[21], (FF, D), scale_ff).astype(jnp.bfloat16),
    }


def layer_norm(x_f32):
    mean_x = jnp.mean(x_f32, axis=-1, keepdims=True)
    centered = x_f32 - mean_x
    var_x = jnp.mean(centered * centered, axis=-1, keepdims=True)
    return centered * lax.rsqrt(var_x + EPS)


def rms_norm(h_lin, gain):
    return h_lin * lax.rsqrt(jnp.mean(h_lin * h_lin, axis=-1, keepdims=True) + EPS) * gain.astype(jnp.float32)


def apply_rope(heads, cos_ang, sin_ang):
    pairs = heads.reshape(heads.shape[:-1] + (HEAD // 2, 2))
    pair_a = pairs[..., 0]
    pair_b = pairs[..., 1]
    turned = jnp.stack([pair_a * cos_ang - pair_b * sin_ang, pair_a * sin_ang + pair_b * cos_ang], axis=-1)
    return turned.reshape(heads.shape)


def project(operand, weight):
    flat = jnp.dot(operand.reshape(-1, operand.shape[-1]), weight, preferred_element_type=jnp.float32)
    return flat.reshape(operand.shape[:-1] + (weight.shape[-1],))


def attend_block(q_blk, k_f32, v_f32):
    scores = jnp.einsum('bqd,bkd->bqk', q_blk.astype(jnp.float32), k_f32) * (HEAD ** -0.5)
    weights = jnp.exp(scores - jnp.max(scores, axis=-1, keepdims=True))
    weighted_v = jnp.einsum('bqk,bkd->bqd', weights.astype(jnp.bfloat16).astype(jnp.float32), v_f32)
    return (weighted_v / jnp.sum(weights, axis=-1, keepdims=True)).astype(jnp.bfloat16)


def reference(tokens, rope_ang, t_emb, block_mod, context, attn_wq, attn_bq, attn_wk, attn_bk, attn_wv, attn_bv, attn_gq, attn_gk, attn_wo, attn_bo, norm3_w, norm3_b, cross_wq, cross_wk, cross_wv, cross_gq, cross_gk, cross_wo, ffn_w1, ffn_w2):
    ada_mod = t_emb + block_mod
    shift1 = ada_mod[:, 0:1]
    scale1 = ada_mod[:, 1:2]
    gate1 = ada_mod[:, 2:3]
    shift2 = ada_mod[:, 3:4]
    scale2 = ada_mod[:, 4:5]
    gate2 = ada_mod[:, 5:6]
    x_res = tokens.astype(jnp.float32)
    y_mod = (layer_norm(x_res) * (1.0 + scale1) + shift1).astype(jnp.bfloat16)
    cos_ang = jnp.cos(rope_ang)[:, None, :]
    sin_ang = jnp.sin(rope_ang)[:, None, :]
    head_shape = (BATCH, SEQ, HEADS, HEAD)
    q_tok = apply_rope(rms_norm(project(y_mod, attn_wq) + attn_bq.astype(jnp.float32), attn_gq).reshape(head_shape), cos_ang, sin_ang).astype(jnp.bfloat16)
    k_tok = apply_rope(rms_norm(project(y_mod, attn_wk) + attn_bk.astype(jnp.float32), attn_gk).reshape(head_shape), cos_ang, sin_ang).astype(jnp.bfloat16)
    v_tok = (project(y_mod, attn_wv) + attn_bv.astype(jnp.float32)).astype(jnp.bfloat16).reshape(head_shape)

    q_heads = jnp.moveaxis(q_tok, 2, 0).reshape(HEADS, BATCH, FRAMES, FRAME_TOK, HEAD)
    k_heads = jnp.moveaxis(k_tok, 2, 0)
    v_heads = jnp.moveaxis(v_tok, 2, 0)

    def self_head(operands):
        q_one, k_one, v_one = operands
        k_f32 = k_one.astype(jnp.float32)
        v_f32 = v_one.astype(jnp.float32)
        return lax.map(lambda q_frame: attend_block(q_frame, k_f32, v_f32), jnp.moveaxis(q_one, 1, 0))

    self_out = lax.map(self_head, (q_heads, k_heads, v_heads))
    attn_out = jnp.transpose(self_out, (2, 1, 3, 0, 4)).reshape(BATCH, SEQ, D)
    x_one = x_res + gate1 * (project(attn_out, attn_wo) + attn_bo.astype(jnp.float32))

    z_norm = (layer_norm(x_one) * norm3_w.astype(jnp.float32) + norm3_b.astype(jnp.float32)).astype(jnp.bfloat16)
    text_shape = (BATCH, TEXT, HEADS, HEAD)
    cross_q = rms_norm(project(z_norm, cross_wq), cross_gq).astype(jnp.bfloat16).reshape(head_shape)
    cross_k = rms_norm(project(context, cross_wk), cross_gk).astype(jnp.bfloat16).reshape(text_shape)
    cross_v = project(context, cross_wv).astype(jnp.bfloat16).reshape(text_shape)

    def cross_head(operands):
        q_one, k_one, v_one = operands
        return attend_block(q_one, k_one.astype(jnp.float32), v_one.astype(jnp.float32))

    cross_out = lax.map(cross_head, (jnp.moveaxis(cross_q, 2, 0), jnp.moveaxis(cross_k, 2, 0), jnp.moveaxis(cross_v, 2, 0)))
    cross_tok = jnp.transpose(cross_out, (1, 2, 0, 3)).reshape(BATCH, SEQ, D)
    x_two = x_one + project(cross_tok, cross_wo)

    def ffn_frame(x_frame):
        hidden = (layer_norm(x_frame) * (1.0 + scale2) + shift2).astype(jnp.bfloat16)
        gelu_out = jax.nn.gelu(project(hidden, ffn_w1), approximate=True).astype(jnp.bfloat16)
        return (x_frame + gate2 * project(gelu_out, ffn_w2)).astype(jnp.bfloat16)

    frames_out = lax.map(ffn_frame, jnp.moveaxis(x_two.reshape(BATCH, FRAMES, FRAME_TOK, D), 1, 0))
    return jnp.moveaxis(frames_out, 0, 1).reshape(BATCH, SEQ, D)
```

```python
import functools

import jax
import jax.numpy as jnp
from jax import lax
from jax.experimental import pallas as pl
from jax.experimental.pallas import tpu as pltpu
from jax.sharding import PartitionSpec as P

EPS = 1e-6
HEAD = 128
LOG2E = 1.4426950408889634
SM_C = (HEAD ** -0.5) * LOG2E
MESH = pl.DeviceIdType.MESH
CHIPS = 8
VMEM_LIMIT = 64 * 1000 * 1024
F32 = jnp.float32
BF16 = jnp.bfloat16

(R_SH1, R_SC1, R_G1, R_SH2, R_SC2, R_G2, R_BQ, R_BK, R_BV, R_BO, R_GQ, R_GK, R_NW, R_NB, R_CGQ, R_CGK) = range(16)


def dot(a, b):
    return jnp.dot(a, b, preferred_element_type=F32)


def dot_nt(a, b):
    return lax.dot_general(a, b, (((1,), (1,)), ((), ())), preferred_element_type=F32)


def my_place():
    uly = lax.axis_index('uly')
    chip = lax.axis_index('sp') * 2 + uly // 2
    return chip, lax.rem(uly, 2)


def device_at(chip, core):
    return {'sp': chip // 2, 'uly': lax.rem(chip, 2) * 2 + core}


def flip(chip, r):
    out = 0
    for bit in (1, 2, 4):
        out = out + lax.rem(chip // bit + r // bit, 2) * bit
    return out


def meet(me, core, sibling):
    barrier = pltpu.get_barrier_semaphore()
    for r in range(1, CHIPS):
        pl.semaphore_signal(barrier, inc=1, device_id=device_at(flip(me, r), core), device_id_type=MESH)
    if sibling:
        pl.semaphore_signal(barrier, inc=1, device_id=device_at(me, 1 - core), device_id_type=MESH)
    return barrier, CHIPS - 1 + int(sibling)


class Ring:
    def __init__(self, slots, sems, phases):
        self.slots, self.sems, self.phases = slots, sems, phases
        self.depth = slots.shape[0]
        self.base = [sum(p[0] for p in phases[:i]) for i in range(len(phases) + 1)]

    def copies(self, phase, tile, slot):
        n, w_ref, k_rows, n_cols, k_parts, shift = self.phases[phase]
        cols = cols_of(lax.rem(tile // k_parts + shift, n // k_parts), n_cols)
        row0 = lax.rem(tile, k_parts) * k_rows
        quarter = k_rows // 4
        out = []
        for c in range(4):
            rows = pl.ds(pl.multiple_of(row0 + c * quarter, quarter), quarter)
            out.append(pltpu.make_async_copy(w_ref.at[rows, cols], self.slots.at[slot, pl.ds(c * quarter, quarter)], self.sems.at[slot]))
        return out

    def start(self, phase, tile):
        slot = lax.rem(self.base[phase] + tile, self.depth)
        for c in self.copies(phase, tile, slot):
            c.start()

    def prime(self):
        for i in range(self.depth - 1):
            self.start(0, i)

    def take(self, phase, tile):
        n = self.phases[phase][0]
        slot = lax.rem(self.base[phase] + tile, self.depth)
        for c in self.copies(phase, tile, slot):
            c.wait()
        ahead = tile + self.depth - 1

        @pl.when(ahead < n)
        def _():
            self.start(phase, ahead)

        if phase + 1 < len(self.phases):
            @pl.when(ahead >= n)
            def _():
                self.start(phase + 1, ahead - n)
        return slot


def cols_of(i, width):
    return pl.ds(pl.multiple_of(i * width, width), width)


def add_squares(ss_ref, rows, acc):
    total = ss_ref[0:rows, :]
    for j in range(acc.shape[1] // 128):
        part = acc[:, j * 128:(j + 1) * 128]
        total = total + part * part
    ss_ref[0:rows, :] = total


def rms_scale(ss_ref, rows, width):
    mean = jnp.sum(ss_ref[0:rows, :], axis=1, keepdims=True) * (1.0 / width)
    ss_ref[0:rows, :] = jnp.broadcast_to(lax.rsqrt(mean + EPS), (rows, 128))


def layer_norm_rows(x_f32, mul, add):
    width = x_f32.shape[1]
    mean = jnp.sum(x_f32, axis=1, keepdims=True) * (1.0 / width)
    centered = x_f32 - mean
    var = jnp.sum(centered * centered, axis=1, keepdims=True) * (1.0 / width)
    return (centered * lax.rsqrt(var + EPS)) * mul + add


def qkv_kernel(x_ref, par_ref, cos_ref, sin_ref, ctx_ref, wv_ref, wk_ref, wq_ref, cwk_ref, cwv_ref,
               q_out, k_out, v_out, ck_out, cv_out,
               y_ref, h_ref, ss_ref, qkv_ref, stage_ref, ring_ref, ring_sem, out_sem, stage_sem, send_sem, recv_sem):
    rows, width = x_ref.shape
    text = ctx_ref.shape[0]
    tn = ring_ref.shape[2]
    nt = width // tn
    part = width // CHIPS
    me, core = my_place()
    barrier, n_signals = meet(me, core, False)
    shift = (nt // 2) * (1 - me // (CHIPS // 2))
    ring = Ring(ring_ref, ring_sem, [(nt, w, width, tn, 1, sh) for w, sh in ((wv_ref, shift), (wk_ref, 0), (wq_ref, 0), (cwk_ref, 0), (cwv_ref, 0))])
    ring.prime()

    def norm_block(i, _):
        r = pl.ds(pl.multiple_of(i * 16, 16), 16)
        x = x_ref[r, :].astype(F32)
        y_ref[r, :] = layer_norm_rows(x, 1.0 + par_ref[R_SC1:R_SC1 + 1, :], par_ref[R_SH1:R_SH1 + 1, :]).astype(BF16)
        return 0

    lax.fori_loop(0, rows // 16, norm_block, 0)
    pl.semaphore_wait(barrier, n_signals)

    def remote(n, dst, r):
        to = flip(me, r)
        return pltpu.make_async_remote_copy(
            src_ref=qkv_ref.at[n, :, cols_of(to, part)], dst_ref=dst.at[cols_of(me, rows)],
            send_sem=send_sem.at[n, r], recv_sem=recv_sem.at[n, r], device_id=device_at(to, core), device_id_type=MESH)

    def local(n, dst):
        return pltpu.make_async_copy(qkv_ref.at[n, :, cols_of(me, part)], dst.at[cols_of(me, rows)], out_sem.at[n])

    def q_copies():
        return [pltpu.make_async_copy(qkv_ref.at[2, :, pl.ds(d * part, part)], q_out.at[d], out_sem.at[2]) for d in range(CHIPS)]

    def v_tile(i, _):
        slot = ring.take(0, i)

        @pl.when(i == nt // 2)
        def _():
            for r in range(CHIPS // 2, CHIPS):
                remote(0, v_out, r).start()

        cols = cols_of(lax.rem(i + shift, nt), tn)
        qkv_ref[0, :, cols] = (dot(y_ref[...], ring_ref[slot]) + par_ref[R_BV:R_BV + 1, cols]).astype(BF16)
        return 0

    lax.fori_loop(0, nt, v_tile, 0)

    def v_rest():
        for r in range(1, CHIPS // 2):
            remote(0, v_out, r).start()
        local(0, v_out).start()

    def k_all():
        for r in range(1, CHIPS):
            remote(1, k_out, r).start()
        local(1, k_out).start()

    def q_all():
        for c in q_copies():
            c.start()

    def normed_phase(phase, n, row_b, row_g, send_last):
        ss_ref[0:rows, :] = jnp.zeros((rows, 128), F32)

        def tile(i, _):
            slot = ring.take(phase, i)
            pl.when(i == 0)(send_last)
            cols = cols_of(i, tn)
            acc = dot(y_ref[...], ring_ref[slot]) + par_ref[row_b:row_b + 1, cols]
            h_ref[0:rows, cols] = acc
            add_squares(ss_ref, rows, acc)
            return 0

        lax.fori_loop(0, nt, tile, 0)
        rms_scale(ss_ref, rows, width)
        even = lax.rem(lax.broadcasted_iota(jnp.int32, (rows, HEAD), 1), 2) == 0

        def head(j, _):
            cols = cols_of(j, HEAD)
            x = (h_ref[0:rows, cols] * ss_ref[0:rows, :]) * par_ref[row_g:row_g + 1, cols]
            other = jnp.where(even, pltpu.roll(x, HEAD - 1, 1), pltpu.roll(x, 1, 1))
            qkv_ref[n, :, cols] = (x * cos_ref[...] + other * sin_ref[...]).astype(BF16)
            return 0

        lax.fori_loop(0, width // HEAD, head, 0)

    normed_phase(1, 1, R_BK, R_GK, v_rest)
    normed_phase(2, 2, R_BQ, R_GQ, k_all)

    def stage_copy(i, slot, dst):
        return pltpu.make_async_copy(stage_ref.at[slot], dst.at[:, cols_of(i, tn)], stage_sem.at[slot])

    ss_ref[...] = jnp.zeros_like(ss_ref)

    def ck_tile(i, _):
        slot = ring.take(3, i)
        pl.when(i == 0)(q_all)
        acc = dot(ctx_ref[...], ring_ref[slot])
        h_ref[:, cols_of(i, tn)] = acc
        add_squares(ss_ref, text, acc)
        return 0

    lax.fori_loop(0, nt, ck_tile, 0)
    rms_scale(ss_ref, text, width)

    def ck_norm(i, _):
        s = lax.rem(i, 2)

        @pl.when(i >= 2)
        def _():
            stage_copy(i, s, ck_out).wait()

        for j in range(tn // HEAD):
            cols = pl.ds(pl.multiple_of(i * tn + j * HEAD, HEAD), HEAD)
            stage_ref[s, :, j * HEAD:(j + 1) * HEAD] = ((h_ref[:, cols] * ss_ref[...]) * par_ref[R_CGK:R_CGK + 1, cols]).astype(BF16)
        stage_copy(i, s, ck_out).start()
        return 0

    lax.fori_loop(0, nt, ck_norm, 0)

    def cv_tile(i, _):
        slot = ring.take(4, i)
        s = lax.rem(nt + i, 2)
        stage_copy(i, s, cv_out).wait()
        stage_ref[s] = dot(ctx_ref[...], ring_ref[slot]).astype(BF16)
        stage_copy(i, s, cv_out).start()
        return 0

    lax.fori_loop(0, nt, cv_tile, 0)
    for i in range(2):
        stage_copy(0, i, cv_out).wait()
    for c in q_copies():
        c.wait()
    for n, dst in ((0, v_out), (1, k_out)):
        local(n, dst).wait()
        for r in range(1, CHIPS):
            remote(n, dst, r).wait()


def any_spec():
    return pl.BlockSpec(memory_space=pl.ANY)


def vmem_spec():
    return pl.BlockSpec(memory_space=pltpu.VMEM)


def qkv_call(x, par, cos, sin, ctx, wv, wk, wq, cwk, cwv, tn):
    rows, width = x.shape
    text = ctx.shape[0]
    part = width // CHIPS
    split = jax.ShapeDtypeStruct((CHIPS, rows, part), BF16)
    gathered = jax.ShapeDtypeStruct((CHIPS * rows, part), BF16)
    flops = 2 * width * width * (3 * rows + 2 * text)
    return pl.pallas_call(
        qkv_kernel,
        out_shape=(split, gathered, gathered, jax.ShapeDtypeStruct((text, width), BF16), jax.ShapeDtypeStruct((text, width), BF16)),
        in_specs=[vmem_spec()] * 5 + [any_spec()] * 5,
        out_specs=[any_spec()] * 5,
        scratch_shapes=[
            pltpu.VMEM((rows, width), BF16),
            pltpu.VMEM((text, width), F32),
            pltpu.VMEM((text, 128), F32),
            pltpu.VMEM((3, rows, width), BF16),
            pltpu.VMEM((2, text, tn), BF16),
            pltpu.VMEM((3, width, tn), BF16),
            pltpu.SemaphoreType.DMA((3,)),
            pltpu.SemaphoreType.DMA((3,)),
            pltpu.SemaphoreType.DMA((2,)),
            pltpu.SemaphoreType.DMA((2, CHIPS)),
            pltpu.SemaphoreType.DMA((2, CHIPS)),
        ],
        compiler_params=pltpu.CompilerParams(vmem_limit_bytes=VMEM_LIMIT, collective_id=0, has_side_effects=True),
        cost_estimate=pl.CostEstimate(flops=flops, bytes_accessed=10 * width * width, transcendentals=0),
        name='qkv',
    )(x, par, cos, sin, ctx, wv, wk, wq, cwk, cwv)


def attend_kernel(q_ref, k_ref, v_ref, o_out, kbuf, vbuf, qbuf, obuf, s0_ref, s1_ref, mx0_ref, mx1_ref,
                  own_sem, pair_send, pair_recv, q_send, q_recv, o_send, o_recv):
    n_heads, keys, _ = kbuf.shape
    half = keys // 2
    rows = qbuf.shape[1]
    blocks = CHIPS * n_heads
    kb = 512 if keys % 512 == 0 else keys
    n_kb = keys // kb
    me, core = my_place()
    barrier, n_signals = meet(me, core, True)

    def own(h):
        return [pltpu.make_async_copy(src.at[:, cols_of(h, HEAD)], dst.at[h, 0:half, :], own_sem.at[n, h])
                for n, (src, dst) in enumerate(((k_ref, kbuf), (v_ref, vbuf)))]

    def pair(h):
        return [pltpu.make_async_remote_copy(
            src_ref=src.at[:, cols_of(h, HEAD)], dst_ref=dst.at[h, pl.ds(half, half), :],
            send_sem=pair_send.at[n, h], recv_sem=pair_recv.at[n, h], device_id=device_at(me, 1 - core), device_id_type=MESH)
            for n, (src, dst) in enumerate(((k_ref, kbuf), (v_ref, vbuf)))]

    def q_local():
        return pltpu.make_async_copy(q_ref.at[me], qbuf.at[0], q_recv.at[0])

    def q_remote(r):
        to = flip(me, r)
        return pltpu.make_async_remote_copy(
            src_ref=q_ref.at[to], dst_ref=qbuf.at[r], send_sem=q_send.at[r], recv_sem=q_recv.at[r],
            device_id=device_at(to, core), device_id_type=MESH)

    def o_local(h):
        cols = cols_of(h, HEAD)
        return pltpu.make_async_copy(obuf.at[0, :, cols], o_out.at[me, :, cols], o_send.at[0, h])

    def o_remote(r, h):
        cols = cols_of(h, HEAD)
        return pltpu.make_async_remote_copy(
            src_ref=obuf.at[r, :, cols], dst_ref=o_out.at[me, :, cols], send_sem=o_send.at[r, h], recv_sem=o_recv.at[r, h],
            device_id=device_at(flip(me, r), core), device_id_type=MESH)

    q_local().start()
    for h in range(n_heads):
        for c in own(h):
            c.start()
    pl.semaphore_wait(barrier, n_signals)
    for c in pair(0):
        c.start()
    for r in range(1, CHIPS):
        q_remote(r).start()
    for h in range(1, n_heads):
        for c in pair(h):
            c.start()

    def send_output(b):
        r, h = b // n_heads, lax.rem(b, n_heads)

        @pl.when(r == 0)
        def _():
            o_local(h).start()

        @pl.when(r > 0)
        def _():
            o_remote(r, h).start()

    def step(i, now, before):
        s_now, mx_now = now
        cur = jnp.minimum(i, blocks - 1)
        r, h = cur // n_heads, lax.rem(cur, n_heads)

        @pl.when(i < n_heads)
        def _():
            for c in own(h):
                c.wait()
            for c in pair(h):
                c.wait_recv()

        @pl.when(i == 0)
        def _():
            q_local().wait()

        @pl.when((i > 0) & (i < blocks) & (h == 0))
        def _():
            q_remote(r).wait_recv()

        if before is not None:
            @pl.when(i >= 2)
            def _():
                send_output(i - 2)

            s_old, mx_old = before
            old_r, old_h = (i - 1) // n_heads, lax.rem(i - 1, n_heads)
            total = jnp.zeros((rows, 128), F32)
            acc = jnp.zeros((rows, HEAD), F32)
        q = qbuf[r, :, cols_of(h, HEAD)]
        mx = None
        for j in range(n_kb):
            s = dot_nt(q, kbuf[h, j * kb:(j + 1) * kb, :])
            s_now[:, j * kb:(j + 1) * kb] = s
            for g in range(kb // 128):
                sg = s[:, g * 128:(g + 1) * 128]
                mx = sg if mx is None else jnp.maximum(mx, sg)
            if before is not None:
                parts = []
                for g in range(kb // 128):
                    c0 = j * kb + g * 128
                    p = jnp.exp2((s_old[:, c0:c0 + 128] - mx_old[...]) * SM_C)
                    total = total + p
                    parts.append(p.astype(BF16))
                acc = acc + dot(jnp.concatenate(parts, axis=1), vbuf[old_h, j * kb:(j + 1) * kb, :])
        mx_now[...] = jnp.broadcast_to(jnp.max(mx, axis=1, keepdims=True), (rows, 128))
        if before is not None:
            obuf[old_r, :, cols_of(old_h, HEAD)] = (acc / jnp.sum(total, axis=1, keepdims=True)).astype(BF16)

    bufs = ((s0_ref, mx0_ref), (s1_ref, mx1_ref))
    step(jnp.int32(0), bufs[0], None)

    def pair_of_steps(t, _):
        step(2 * t + 1, bufs[1], bufs[0])
        step(2 * t + 2, bufs[0], bufs[1])
        return 0

    lax.fori_loop(0, blocks // 2, pair_of_steps, 0)
    send_output(jnp.int32(blocks - 1))

    for h in range(n_heads):
        for c in pair(h):
            c.wait_send()
        o_local(h).wait()

    def drain(r, _):
        q_remote(r).wait_send()
        for h in range(n_heads):
            o_remote(r, h).wait()
        return 0

    lax.fori_loop(1, CHIPS, drain, 0)


def attend_call(q, k, v):
    _, rows, part = q.shape
    half = k.shape[0]
    n_heads = part // HEAD
    flops = 8 * half * half * part
    return pl.pallas_call(
        attend_kernel,
        out_shape=jax.ShapeDtypeStruct((CHIPS, rows, part), BF16),
        in_specs=[any_spec()] * 3,
        out_specs=any_spec(),
        scratch_shapes=[
            pltpu.VMEM((n_heads, 2 * half, HEAD), BF16),
            pltpu.VMEM((n_heads, 2 * half, HEAD), BF16),
            pltpu.VMEM((CHIPS, rows, part), BF16),
            pltpu.VMEM((CHIPS, rows, part), BF16),
            pltpu.VMEM((rows, 2 * half), F32),
            pltpu.VMEM((rows, 2 * half), F32),
            pltpu.VMEM((rows, 128), F32),
            pltpu.VMEM((rows, 128), F32),
            pltpu.SemaphoreType.DMA((2, n_heads)),
            pltpu.SemaphoreType.DMA((2, n_heads)),
            pltpu.SemaphoreType.DMA((2, n_heads)),
            pltpu.SemaphoreType.DMA((CHIPS,)),
            pltpu.SemaphoreType.DMA((CHIPS,)),
            pltpu.SemaphoreType.DMA((CHIPS, n_heads)),
            pltpu.SemaphoreType.DMA((CHIPS, n_heads)),
        ],
        compiler_params=pltpu.CompilerParams(vmem_limit_bytes=VMEM_LIMIT, collective_id=1, has_side_effects=True),
        cost_estimate=pl.CostEstimate(flops=flops, bytes_accessed=8 * half * part, transcendentals=2 * half * half * n_heads),
        name='attend',
    )(q, k, v)


def tail_kernel(x_ref, par_ref, o_ref, ck_ref, cv_ref, wo_ref, cwq_ref, cwo_ref, w1_ref, w2_ref, out_ref,
                a_ref, b_ref, xf_ref, h_ref, u_ref, ss_ref, kbuf, vbuf, stage_ref, ring_ref,
                ring_sem, in_sem, kv_sem, stage_sem):
    rows, width = x_ref.shape
    ff = u_ref.shape[1]
    tn = ring_ref.shape[2]
    nt = width // tn
    n_ff = ff // tn
    k_parts = 1
    while ff // k_parts > width or ff % k_parts:
        k_parts += 1
    kc = ff // k_parts
    part = width // CHIPS
    ring = Ring(ring_ref, ring_sem, [
        (nt, wo_ref, width, tn, 1, 0), (nt, cwq_ref, width, tn, 1, 0), (nt, cwo_ref, width, tn, 1, 0),
        (n_ff, w1_ref, width, tn, 1, 0), (nt * k_parts, w2_ref, kc, tn, k_parts, 0)])
    o_copies = [pltpu.make_async_copy(o_ref.at[d], a_ref.at[:, pl.ds(d * part, part)], in_sem) for d in range(CHIPS)]
    for c in o_copies:
        c.start()
    ring.prime()
    for c in o_copies:
        c.wait()

    def o_tile(i, _):
        slot = ring.take(0, i)
        cols = cols_of(i, tn)
        acc = dot(a_ref[...], ring_ref[slot]) + par_ref[R_BO:R_BO + 1, cols]
        xf_ref[:, cols] = x_ref[:, cols].astype(F32) + par_ref[R_G1:R_G1 + 1, cols] * acc
        return 0

    lax.fori_loop(0, nt, o_tile, 0)

    def norm_to(dst, mul, add):
        def block(i, _):
            r = pl.ds(pl.multiple_of(i * 16, 16), 16)
            dst[r, :] = layer_norm_rows(xf_ref[r, :], mul(), add()).astype(BF16)
            return 0

        lax.fori_loop(0, rows // 16, block, 0)

    norm_to(b_ref, lambda: par_ref[R_NW:R_NW + 1, :], lambda: par_ref[R_NB:R_NB + 1, :])
    ss_ref[...] = jnp.zeros_like(ss_ref)

    def cq_tile(i, _):
        slot = ring.take(1, i)
        acc = dot(b_ref[...], ring_ref[slot])
        h_ref[:, cols_of(i, tn)] = acc
        add_squares(ss_ref, rows, acc)
        return 0

    lax.fori_loop(0, nt, cq_tile, 0)
    rms_scale(ss_ref, rows, width)

    def cq_head(j, _):
        cols = cols_of(j, HEAD)
        a_ref[:, cols] = ((h_ref[:, cols] * ss_ref[...]) * par_ref[R_CGQ:R_CGQ + 1, cols]).astype(BF16)
        return 0

    gw = kbuf.shape[2]
    n_groups = width // gw
    heads = gw // HEAD

    def kv_loads(g, slot):
        cols = cols_of(g, gw)
        return (pltpu.make_async_copy(ck_ref.at[:, cols], kbuf.at[slot], kv_sem.at[0, slot]),
                pltpu.make_async_copy(cv_ref.at[:, cols], vbuf.at[slot], kv_sem.at[1, slot]))

    for c in kv_loads(0, 0):
        c.start()
    lax.fori_loop(0, width // HEAD, cq_head, 0)

    def cross_group(g, _):
        slot = lax.rem(g, 2)
        for c in kv_loads(g, slot):
            c.wait()

        @pl.when(g + 1 < n_groups)
        def _():
            for c in kv_loads(g + 1, 1 - slot):
                c.start()

        for j in range(heads):
            cols = pl.ds(pl.multiple_of(g * gw + j * HEAD, HEAD), HEAD)
            hs = slice(j * HEAD, (j + 1) * HEAD)
            s = dot_nt(a_ref[:, cols], kbuf[slot, :, hs])
            m = jnp.max(s, axis=1, keepdims=True)
            p = jnp.exp2((s - m) * SM_C)
            total = jnp.sum(p, axis=1, keepdims=True)
            b_ref[:, cols] = (dot(p.astype(BF16), vbuf[slot, :, hs]) / total).astype(BF16)
        return 0

    lax.fori_loop(0, n_groups, cross_group, 0)

    def co_tile(i, _):
        slot = ring.take(2, i)
        cols = cols_of(i, tn)
        xf_ref[:, cols] = xf_ref[:, cols] + dot(b_ref[...], ring_ref[slot])
        return 0

    lax.fori_loop(0, nt, co_tile, 0)
    norm_to(a_ref, lambda: 1.0 + par_ref[R_SC2:R_SC2 + 1, :], lambda: par_ref[R_SH2:R_SH2 + 1, :])

    def f1_tile(i, _):
        slot = ring.take(3, i)
        acc = dot(a_ref[...], ring_ref[slot])
        u_ref[:, cols_of(i, tn)] = jax.nn.gelu(acc, approximate=True).astype(BF16)
        return 0

    lax.fori_loop(0, n_ff, f1_tile, 0)

    def stage_copy(i, slot):
        return pltpu.make_async_copy(stage_ref.at[slot], out_ref.at[:, cols_of(i, tn)], stage_sem.at[slot])

    def f2_tile(i, _):
        s = lax.rem(i, 2)

        @pl.when(i >= 2)
        def _():
            stage_copy(i, s).wait()

        acc = None
        for c in range(k_parts):
            slot = ring.take(4, i * k_parts + c)
            term = dot(u_ref[:, c * kc:(c + 1) * kc], ring_ref[slot, 0:kc, :])
            acc = term if acc is None else acc + term
        cols = cols_of(i, tn)
        stage_ref[s] = (xf_ref[:, cols] + par_ref[R_G2:R_G2 + 1, cols] * acc).astype(BF16)
        stage_copy(i, s).start()
        return 0

    lax.fori_loop(0, nt, f2_tile, 0)
    for i in range(2):
        stage_copy(0, i).wait()


def tail_call(x, par, o, ck, cv, wo, cwq, cwo, w1, w2, tn):
    rows, width = x.shape
    text = ck.shape[0]
    ff = w1.shape[1]
    flops = 2 * rows * width * (3 * width + 2 * ff) + 4 * rows * text * width
    return pl.pallas_call(
        tail_kernel,
        out_shape=jax.ShapeDtypeStruct((rows, width), BF16),
        in_specs=[vmem_spec()] * 2 + [any_spec()] * 8,
        out_specs=any_spec(),
        scratch_shapes=[
            pltpu.VMEM((rows, width), BF16),
            pltpu.VMEM((rows, width), BF16),
            pltpu.VMEM((rows, width), F32),
            pltpu.VMEM((rows, width), F32),
            pltpu.VMEM((rows, ff), BF16),
            pltpu.VMEM((rows, 128), F32),
            pltpu.VMEM((2, text, 4 * HEAD), BF16),
            pltpu.VMEM((2, text, 4 * HEAD), BF16),
            pltpu.VMEM((2, rows, tn), BF16),
            pltpu.VMEM((3, width, tn), BF16),
            pltpu.SemaphoreType.DMA((3,)),
            pltpu.SemaphoreType.DMA,
            pltpu.SemaphoreType.DMA((2, 2)),
            pltpu.SemaphoreType.DMA((2,)),
        ],
        compiler_params=pltpu.CompilerParams(vmem_limit_bytes=VMEM_LIMIT),
        cost_estimate=pl.CostEstimate(flops=flops, bytes_accessed=2 * width * (3 * width + 2 * ff), transcendentals=rows * ff),
        name='tail',
    )(x, par, o, ck, cv, wo, cwq, cwo, w1, w2)


def solution(mesh):
    tok_spec = P('dp', ('sp', 'uly'), None)
    batch_spec = P('dp', None, None)

    def local_block(tokens, rope_ang, t_emb, block_mod, context, attn_wq, attn_bq, attn_wk, attn_bk, attn_wv, attn_bv, attn_gq, attn_gk, attn_wo, attn_bo, norm3_w, norm3_b, cross_wq, cross_wk, cross_wv, cross_gq, cross_gk, cross_wo, ffn_w1, ffn_w2):
        x = tokens[0]
        tn = 512
        vectors = jnp.stack([attn_bq, attn_bk, attn_bv, attn_bo, attn_gq, attn_gk, norm3_w, norm3_b, cross_gq, cross_gk]).astype(F32)
        par = jnp.concatenate([t_emb[0] + block_mod[0], vectors], axis=0)
        lane = jnp.arange(HEAD)
        spread = (lane[None, :] // 2 == jnp.arange(HEAD // 2)[:, None]).astype(F32)
        sign = jnp.where(lane % 2 == 0, -1.0, 1.0).astype(F32)
        cos = jnp.dot(jnp.cos(rope_ang), spread, precision=lax.Precision.HIGHEST)
        sin = jnp.dot(jnp.sin(rope_ang), spread * sign[None, :], precision=lax.Precision.HIGHEST)
        q, k, v, ck, cv = qkv_call(x, par, cos, sin, context[0], attn_wv, attn_wk, attn_wq, cross_wk, cross_wv, tn)
        o_own = attend_call(q, k, v)
        out = tail_call(x, par, o_own, ck, cv, attn_wo, cross_wq, cross_wo, ffn_w1, ffn_w2, tn)
        return out[None]

    in_specs = (tok_spec, P(('sp', 'uly'), None), batch_spec, P(), batch_spec) + (P(),) * 20
    return jax.shard_map(local_block, mesh=mesh, in_specs=in_specs, out_specs=tok_spec, check_vma=False)
```

```python
import functools

import jax
import jax.numpy as jnp
from jax import lax
from jax.experimental import pallas as pl
from jax.experimental.pallas import tpu as pltpu
from jax.sharding import PartitionSpec as P

EPS = 1e-6
HEAD = 128
LOG2E = 1.4426950408889634
SM_C = (HEAD ** -0.5) * LOG2E
MESH = pl.DeviceIdType.MESH
CHIPS = 8
VMEM_LIMIT = 64 * 1000 * 1024
F32 = jnp.float32
BF16 = jnp.bfloat16

SH1, SC1, G1, SH2, SC2, G2 = range(6)


def dot(a, b):
    return jnp.dot(a, b, preferred_element_type=F32)


def dot_nt(a, b):
    return lax.dot_general(a, b, (((1,), (1,)), ((), ())), preferred_element_type=F32)


def my_place():
    uly = lax.axis_index('uly')
    chip = lax.axis_index('sp') * 2 + uly // 2
    return chip, lax.rem(uly, 2)


def device_at(chip, core):
    return {'sp': chip // 2, 'uly': lax.rem(chip, 2) * 2 + core}


def flip(chip, r):
    out = 0
    for bit in (1, 2, 4):
        out = out + lax.rem(chip // bit + r // bit, 2) * bit
    return out


def meet(me, core, sibling):
    barrier = pltpu.get_barrier_semaphore()
    for r in range(1, CHIPS):
        pl.semaphore_signal(barrier, inc=1, device_id=device_at(flip(me, r), core), device_id_type=MESH)
    if sibling:
        pl.semaphore_signal(barrier, inc=1, device_id=device_at(me, 1 - core), device_id_type=MESH)
    return barrier, CHIPS - 1 + int(sibling)


class Ring:
    def __init__(self, slots, sems, phases):
        self.slots, self.sems, self.phases = slots, sems, phases
        self.depth = slots.shape[0]
        self.base = [sum(p[0] for p in phases[:i]) for i in range(len(phases) + 1)]

    def slot(self, phase, tile):
        return lax.rem(self.base[phase] + tile, self.depth)

    def copies(self, phase, tile):
        n, w_ref, k_rows, n_cols, k_parts, shift = self.phases[phase]
        slot = self.slot(phase, tile)
        cols = cols_of(lax.rem(tile // k_parts + shift, n // k_parts), n_cols)
        row0 = lax.rem(tile, k_parts) * k_rows
        quarter = k_rows // 4
        out = []
        for c in range(4):
            rows = pl.ds(pl.multiple_of(row0 + c * quarter, quarter), quarter)
            out.append(pltpu.make_async_copy(w_ref.at[rows, cols], self.slots.at[slot, pl.ds(c * quarter, quarter)], self.sems.at[slot]))
        return out

    def start(self, phase, tile):
        for c in self.copies(phase, tile):
            c.start()

    def prime(self):
        for i in range(self.depth):
            if i < self.phases[0][0]:
                self.start(0, i)
            else:
                self.start(1, i - self.phases[0][0])

    def wait(self, phase, tile):
        for c in self.copies(phase, tile):
            c.wait()
        return self.slot(phase, tile)

    def refill(self, phase, tile):
        n = self.phases[phase][0]
        ahead = tile + self.depth

        @pl.when(ahead < n)
        def _():
            self.start(phase, ahead)

        if phase + 1 < len(self.phases):
            @pl.when(ahead >= n)
            def _():
                self.start(phase + 1, ahead - n)


def cols_of(i, width):
    return pl.ds(pl.multiple_of(i * width, width), width)


def groups(acc):
    return [acc[:, g * 128:(g + 1) * 128] for g in range(acc.shape[1] // 128)]


def add_lanes(ref, rows, acc, squares):
    total = ref[0:rows, :]
    for part in groups(acc):
        total = total + (part * part if squares else part)
    ref[0:rows, :] = total


def lane_mean(ref, rows, width):
    return jnp.broadcast_to(jnp.sum(ref[0:rows, :], axis=1, keepdims=True) * (1.0 / width), (rows, 128))


def rms_scale(ss_ref, rows, width):
    ss_ref[0:rows, :] = lax.rsqrt(lane_mean(ss_ref, rows, width) + EPS)


def load_vectors(vec_ref, refs):
    for n, ref in enumerate(refs):
        vec_ref[n] = ref[...].astype(F32)


def layer_norm(load, store, mul, add, rows, width, sum_ref, mean_ref, have_sum):
    step = 4 if width % 512 == 0 else 1
    n = width // 128 // step

    def sums(j, _):
        total = sum_ref[0:rows, :]
        for g in range(step):
            total = total + load(j * step + g)
        sum_ref[0:rows, :] = total
        return 0

    if not have_sum:
        sum_ref[0:rows, :] = jnp.zeros((rows, 128), F32)
        lax.fori_loop(0, n, sums, 0)
    mean_ref[...] = lane_mean(sum_ref, rows, width)
    sum_ref[0:rows, :] = jnp.zeros((rows, 128), F32)

    def squares(j, _):
        total = sum_ref[0:rows, :]
        for g in range(step):
            d = load(j * step + g) - mean_ref[...]
            total = total + d * d
        sum_ref[0:rows, :] = total
        return 0

    lax.fori_loop(0, n, squares, 0)
    rms_scale(sum_ref, rows, width)

    def apply(j, _):
        for g in range(step):
            k = j * step + g
            store(k, ((load(k) - mean_ref[...]) * sum_ref[0:rows, :]) * mul(k) + add(k))
        return 0

    lax.fori_loop(0, n, apply, 0)


def qkv_kernel(x_ref, te_ref, bm_ref, ang_ref, bq_ref, bk_ref, bv_ref, gq_ref, gk_ref, cgk_ref,
               ctx_hbm, wv_ref, wk_ref, wq_ref, cwk_ref,
               q_out, k_out, v_out, ck_out,
               y_ref, h_ref, ss_ref, mean_ref, cos_ref, sin_ref, vec_ref, mod_ref, qkv_ref, ctx_ref, stage_ref, ring_ref,
               ring_sem, out_sem, ctx_sem, stage_sem, send_sem, recv_sem):
    rows, width = x_ref.shape
    text = ctx_ref.shape[0]
    tn = ring_ref.shape[2]
    per = tn // 128
    nt = width // tn
    part = width // CHIPS
    me, core = my_place()
    barrier, n_signals = meet(me, core, False)
    far = (CHIPS // 2) * (1 - me // (CHIPS // 2))
    shift = far * part // tn
    ring = Ring(ring_ref, ring_sem, [(nt, w, width, tn, 1, sh) for w, sh in ((wv_ref, shift), (wk_ref, 0), (wq_ref, 0), (cwk_ref, 0))])
    ring.prime()
    ctx_copy = pltpu.make_async_copy(ctx_hbm, ctx_ref, ctx_sem)
    ctx_copy.start()
    load_vectors(vec_ref, (bq_ref, bk_ref, bv_ref, gq_ref, gk_ref, cgk_ref))
    BQ, BK, BV, GQ, GK, CGK = range(6)
    mod_ref[...] = te_ref[...] + bm_ref[...]

    def vec(n, k):
        return vec_ref[n, pl.ds(k, 1), :]

    def store_y(k, val):
        y_ref[:, cols_of(k, 128)] = val.astype(BF16)

    layer_norm(lambda k: x_ref[:, cols_of(k, 128)].astype(F32), store_y,
               lambda k: 1.0 + mod_ref[SC1:SC1 + 1, cols_of(k, 128)], lambda k: mod_ref[SH1:SH1 + 1, cols_of(k, 128)],
               rows, width, ss_ref, mean_ref, False)
    pl.semaphore_wait(barrier, n_signals)

    def remote(n, dst, r):
        to = flip(me, r)
        return pltpu.make_async_remote_copy(
            src_ref=qkv_ref.at[n, :, cols_of(to, part)], dst_ref=dst.at[cols_of(me, rows)],
            send_sem=send_sem.at[n, r], recv_sem=recv_sem.at[n, r], device_id=device_at(to, core), device_id_type=MESH)

    def local(n, dst):
        return pltpu.make_async_copy(qkv_ref.at[n, :, cols_of(me, part)], dst.at[cols_of(me, rows)], out_sem.at[n])

    def q_copies():
        return [pltpu.make_async_copy(qkv_ref.at[2, :, pl.ds(d * part, part)], q_out.at[d], out_sem.at[2]) for d in range(CHIPS)]

    def v_tile(i, _):
        slot = ring.wait(0, i)
        for j in range(CHIPS // 2):
            @pl.when(i == -(-part * (j + 1) // tn))
            def _():
                remote(0, v_out, flip(me, far + j)).start()

        ct = lax.rem(i + shift, nt)
        for g, a in enumerate(groups(dot(y_ref[...], ring_ref[slot]))):
            k = ct * per + g
            qkv_ref[0, :, cols_of(k, 128)] = (a + vec(BV, k)).astype(BF16)
        ring.refill(0, i)
        return 0

    lax.fori_loop(0, nt, v_tile, 0)

    def v_rest():
        for r in range(1, CHIPS // 2):
            remote(0, v_out, r).start()
        local(0, v_out).start()
        ang = jnp.concatenate([ang_ref[...], ang_ref[...]], axis=1)
        lane = lax.broadcasted_iota(jnp.int32, (rows, HEAD), 1)
        spread = jnp.take_along_axis(ang, lane // 2, axis=1)
        cos_ref[...] = jnp.cos(spread)
        sin_ref[...] = jnp.where(lax.rem(lane, 2) == 0, -1.0, 1.0) * jnp.sin(spread)

    def k_all():
        for r in range(CHIPS - 1, 0, -1):
            remote(1, k_out, r).start()
        local(1, k_out).start()

    def q_all():
        for c in q_copies():
            c.start()
        ctx_copy.wait()

    def normed_phase(phase, n, b, gain, send_last):
        ss_ref[0:rows, :] = jnp.zeros((rows, 128), F32)

        def tile(i, _):
            slot = ring.wait(phase, i)
            pl.when(i == 0)(send_last)
            total = ss_ref[0:rows, :]
            for g, a in enumerate(groups(dot(y_ref[...], ring_ref[slot]))):
                k = i * per + g
                a = a + vec(b, k)
                h_ref[0:rows, cols_of(k, 128)] = a
                total = total + a * a
            ss_ref[0:rows, :] = total
            ring.refill(phase, i)
            return 0

        lax.fori_loop(0, nt, tile, 0)
        rms_scale(ss_ref, rows, width)
        even = lax.rem(lax.broadcasted_iota(jnp.int32, (rows, HEAD), 1), 2) == 0

        def head(j, _):
            cols = cols_of(j, HEAD)
            x = (h_ref[0:rows, cols] * ss_ref[0:rows, :]) * vec(gain, j)
            other = jnp.where(even, pltpu.roll(x, HEAD - 1, 1), pltpu.roll(x, 1, 1))
            qkv_ref[n, :, cols] = (x * cos_ref[...] + other * sin_ref[...]).astype(BF16)
            return 0

        lax.fori_loop(0, width // HEAD, head, 0)

    normed_phase(1, 1, BK, GK, v_rest)
    normed_phase(2, 2, BQ, GQ, k_all)

    def stage_copy(i, slot):
        return pltpu.make_async_copy(stage_ref.at[slot], ck_out.at[:, cols_of(i, tn)], stage_sem.at[slot])

    ss_ref[...] = jnp.zeros_like(ss_ref)

    def ck_tile(i, _):
        slot = ring.wait(3, i)
        pl.when(i == 0)(q_all)
        acc = dot(ctx_ref[...], ring_ref[slot])
        h_ref[:, cols_of(i, tn)] = acc
        add_lanes(ss_ref, text, acc, True)
        ring.refill(3, i)
        return 0

    lax.fori_loop(0, nt, ck_tile, 0)
    rms_scale(ss_ref, text, width)

    def ck_norm(i, _):
        s = lax.rem(i, 2)

        @pl.when(i >= 2)
        def _():
            stage_copy(i, s).wait()

        for j in range(per):
            k = i * per + j
            stage_ref[s, :, j * HEAD:(j + 1) * HEAD] = ((h_ref[:, cols_of(k, 128)] * ss_ref[...]) * vec(CGK, k)).astype(BF16)
        stage_copy(i, s).start()
        return 0

    lax.fori_loop(0, nt, ck_norm, 0)
    for i in range(2):
        stage_copy(0, i).wait()
    for c in q_copies():
        c.wait()
    for n, dst in ((0, v_out), (1, k_out)):
        local(n, dst).wait()
        for r in range(1, CHIPS):
            remote(n, dst, r).wait()


def any_spec():
    return pl.BlockSpec(memory_space=pl.ANY)


def vmem_spec():
    return pl.BlockSpec(memory_space=pltpu.VMEM)


def qkv_call(x, te, bm, ang, vectors, ctx, wv, wk, wq, cwk, tn):
    rows, width = x.shape
    text = ctx.shape[0]
    part = width // CHIPS
    split = jax.ShapeDtypeStruct((CHIPS, rows, part), BF16)
    gathered = jax.ShapeDtypeStruct((CHIPS * rows, part), BF16)
    flops = 2 * width * width * (3 * rows + text)
    return pl.pallas_call(
        qkv_kernel,
        out_shape=(split, gathered, gathered, jax.ShapeDtypeStruct((text, width), BF16)),
        in_specs=[vmem_spec()] * (4 + len(vectors)) + [any_spec()] * 5,
        out_specs=[any_spec()] * 4,
        scratch_shapes=[
            pltpu.VMEM((rows, width), BF16),
            pltpu.VMEM((text, width), F32),
            pltpu.VMEM((text, 128), F32),
            pltpu.VMEM((rows, 128), F32),
            pltpu.VMEM((rows, 128), F32),
            pltpu.VMEM((rows, 128), F32),
            pltpu.VMEM((len(vectors), width // 128, 128), F32),
            pltpu.VMEM(te.shape, F32),
            pltpu.VMEM((3, rows, width), BF16),
            pltpu.VMEM((text, width), BF16),
            pltpu.VMEM((2, text, tn), BF16),
            pltpu.VMEM((3, width, tn), BF16),
            pltpu.SemaphoreType.DMA((3,)),
            pltpu.SemaphoreType.DMA((3,)),
            pltpu.SemaphoreType.DMA,
            pltpu.SemaphoreType.DMA((2,)),
            pltpu.SemaphoreType.DMA((2, CHIPS)),
            pltpu.SemaphoreType.DMA((2, CHIPS)),
        ],
        compiler_params=pltpu.CompilerParams(vmem_limit_bytes=VMEM_LIMIT, collective_id=0, has_side_effects=True),
        cost_estimate=pl.CostEstimate(flops=flops, bytes_accessed=8 * width * width, transcendentals=0),
        name='qkv',
    )(x, te, bm, ang, *vectors, ctx, wv, wk, wq, cwk)


def attend_kernel(q_ref, k_ref, v_ref, ctx_hbm, cwv_ref, o_out, cv_out,
                  kbuf, vbuf, qbuf, obuf, s0_ref, s1_ref, mx0_ref, mx1_ref, ctx_ref, stage_ref, ring_ref,
                  own_sem, pair_send, pair_recv, q_send, q_recv, o_send, o_recv, ctx_sem, stage_sem, ring_sem):
    n_heads, keys, _ = kbuf.shape
    half = keys // 2
    rows = qbuf.shape[1]
    blocks = CHIPS * n_heads
    kb = 512 if keys % 512 == 0 else keys
    n_kb = keys // kb
    me, core = my_place()
    barrier, n_signals = meet(me, core, True)

    def own(h):
        return [pltpu.make_async_copy(src.at[:, cols_of(h, HEAD)], dst.at[h, 0:half, :], own_sem.at[n, h])
                for n, (src, dst) in enumerate(((k_ref, kbuf), (v_ref, vbuf)))]

    def pair(h):
        return [pltpu.make_async_remote_copy(
            src_ref=src.at[:, cols_of(h, HEAD)], dst_ref=dst.at[h, pl.ds(half, half), :],
            send_sem=pair_send.at[n, h], recv_sem=pair_recv.at[n, h], device_id=device_at(me, 1 - core), device_id_type=MESH)
            for n, (src, dst) in enumerate(((k_ref, kbuf), (v_ref, vbuf)))]

    def q_local():
        return pltpu.make_async_copy(q_ref.at[me], qbuf.at[0], q_recv.at[0])

    def q_remote(r):
        to = flip(me, r)
        return pltpu.make_async_remote_copy(
            src_ref=q_ref.at[to], dst_ref=qbuf.at[r], send_sem=q_send.at[r], recv_sem=q_recv.at[r],
            device_id=device_at(to, core), device_id_type=MESH)

    def o_local(h):
        cols = cols_of(h, HEAD)
        return pltpu.make_async_copy(obuf.at[0, :, cols], o_out.at[me, :, cols], o_send.at[0, h])

    def o_remote(r, h):
        cols = cols_of(h, HEAD)
        return pltpu.make_async_remote_copy(
            src_ref=obuf.at[r, :, cols], dst_ref=o_out.at[me, :, cols], send_sem=o_send.at[r, h], recv_sem=o_recv.at[r, h],
            device_id=device_at(flip(me, r), core), device_id_type=MESH)

    q_local().start()
    for h in range(n_heads):
        for c in own(h):
            c.start()
    pl.semaphore_wait(barrier, n_signals)
    for c in pair(0):
        c.start()
    for r in range(1, CHIPS):
        q_remote(r).start()
    for h in range(1, n_heads):
        for c in pair(h):
            c.start()
    tn = ring_ref.shape[2]
    nt = ring_ref.shape[1] // tn
    ring = Ring(ring_ref, ring_sem, [(nt, cwv_ref, ring_ref.shape[1], tn, 1, 0)])
    ring.prime()
    ctx_copy = pltpu.make_async_copy(ctx_hbm, ctx_ref, ctx_sem)
    ctx_copy.start()

    def stage_copy(i, slot):
        return pltpu.make_async_copy(stage_ref.at[slot], cv_out.at[:, cols_of(i, tn)], stage_sem.at[slot])

    def cv_tile(i):
        slot = ring.wait(0, i)
        s = lax.rem(i, 2)

        @pl.when(i == 0)
        def _():
            ctx_copy.wait()

        @pl.when(i >= 2)
        def _():
            stage_copy(i, s).wait()

        stage_ref[s] = dot(ctx_ref[...], ring_ref[slot]).astype(BF16)
        stage_copy(i, s).start()
        ring.refill(0, i)

    def send_output(b):
        r, h = b // n_heads, lax.rem(b, n_heads)

        @pl.when(r == 0)
        def _():
            o_local(h).start()

        @pl.when(r > 0)
        def _():
            o_remote(r, h).start()

    def step(i, now, before):
        s_now, mx_now = now
        cur = jnp.minimum(i, blocks - 1)
        r, h = cur // n_heads, lax.rem(cur, n_heads)

        @pl.when(i < n_heads)
        def _():
            for c in own(h):
                c.wait()
            for c in pair(h):
                c.wait_recv()

        @pl.when(i == 0)
        def _():
            q_local().wait()

        @pl.when((i > 0) & (i < blocks) & (h == 0))
        def _():
            q_remote(r).wait_recv()

        if before is not None:
            @pl.when(i >= 2)
            def _():
                send_output(i - 2)

            s_old, mx_old = before
            old_r, old_h = (i - 1) // n_heads, lax.rem(i - 1, n_heads)
            total = jnp.zeros((rows, 128), F32)
            acc = jnp.zeros((rows, HEAD), F32)
        q = qbuf[r, :, cols_of(h, HEAD)]
        mx = None
        for j in range(n_kb):
            s = dot_nt(q, kbuf[h, j * kb:(j + 1) * kb, :])
            s_now[:, j * kb:(j + 1) * kb] = s
            for g in range(kb // 128):
                sg = s[:, g * 128:(g + 1) * 128]
                mx = sg if mx is None else jnp.maximum(mx, sg)
            if before is not None:
                parts = []
                for g in range(kb // 128):
                    c0 = j * kb + g * 128
                    p = jnp.exp2((s_old[:, c0:c0 + 128] - mx_old[...]) * SM_C)
                    total = total + p
                    parts.append(p.astype(BF16))
                acc = acc + dot(jnp.concatenate(parts, axis=1), vbuf[old_h, j * kb:(j + 1) * kb, :])
        mx_now[...] = jnp.broadcast_to(jnp.max(mx, axis=1, keepdims=True), (rows, 128))
        if before is not None:
            obuf[old_r, :, cols_of(old_h, HEAD)] = (acc / jnp.sum(total, axis=1, keepdims=True)).astype(BF16)

    bufs = ((s0_ref, mx0_ref), (s1_ref, mx1_ref))
    step(jnp.int32(0), bufs[0], None)

    def pair_of_steps(t, _):
        step(2 * t + 1, bufs[1], bufs[0])
        step(2 * t + 2, bufs[0], bufs[1])

        @pl.when((lax.rem(t, every) == 0) & (t < nt * every))
        def _():
            cv_tile(t // every)

        return 0

    every = blocks // 2 // nt
    lax.fori_loop(0, blocks // 2, pair_of_steps, 0)
    send_output(jnp.int32(blocks - 1))
    for i in range(2):
        stage_copy(0, i).wait()

    for h in range(n_heads):
        for c in pair(h):
            c.wait_send()
        o_local(h).wait()

    def drain(r, _):
        q_remote(r).wait_send()
        for h in range(n_heads):
            o_remote(r, h).wait()
        return 0

    lax.fori_loop(1, CHIPS, drain, 0)


def attend_call(q, k, v, ctx, cwv, tn):
    _, rows, part = q.shape
    half = k.shape[0]
    n_heads = part // HEAD
    text, width = ctx.shape
    flops = 8 * half * half * part + 2 * text * width * width
    return pl.pallas_call(
        attend_kernel,
        out_shape=(jax.ShapeDtypeStruct((CHIPS, rows, part), BF16), jax.ShapeDtypeStruct((text, width), BF16)),
        in_specs=[any_spec()] * 5,
        out_specs=[any_spec()] * 2,
        scratch_shapes=[
            pltpu.VMEM((n_heads, 2 * half, HEAD), BF16),
            pltpu.VMEM((n_heads, 2 * half, HEAD), BF16),
            pltpu.VMEM((CHIPS, rows, part), BF16),
            pltpu.VMEM((CHIPS, rows, part), BF16),
            pltpu.VMEM((rows, 2 * half), F32),
            pltpu.VMEM((rows, 2 * half), F32),
            pltpu.VMEM((rows, 128), F32),
            pltpu.VMEM((rows, 128), F32),
            pltpu.VMEM((text, width), BF16),
            pltpu.VMEM((2, text, tn), BF16),
            pltpu.VMEM((2, width, tn), BF16),
            pltpu.SemaphoreType.DMA((2, n_heads)),
            pltpu.SemaphoreType.DMA((2, n_heads)),
            pltpu.SemaphoreType.DMA((2, n_heads)),
            pltpu.SemaphoreType.DMA((CHIPS,)),
            pltpu.SemaphoreType.DMA((CHIPS,)),
            pltpu.SemaphoreType.DMA((CHIPS, n_heads)),
            pltpu.SemaphoreType.DMA((CHIPS, n_heads)),
            pltpu.SemaphoreType.DMA,
            pltpu.SemaphoreType.DMA((2,)),
            pltpu.SemaphoreType.DMA((2,)),
        ],
        compiler_params=pltpu.CompilerParams(vmem_limit_bytes=VMEM_LIMIT, collective_id=1, has_side_effects=True),
        cost_estimate=pl.CostEstimate(flops=flops, bytes_accessed=8 * half * part + 2 * width * width, transcendentals=2 * half * half * n_heads),
        name='attend',
    )(q, k, v, ctx, cwv)


def tail_kernel(te_ref, bm_ref, bo_ref, nw_ref, nb_ref, cgq_ref, x_hbm, o_ref, ck_ref, cv_ref, wo_ref, cwq_ref, cwo_ref, w1_ref, w2_ref,
                out_ref, a_ref, b_ref, xf_ref, h_ref, u_ref, ss_ref, mean_ref, vec_ref, mod_ref, kbuf, vbuf,
                s0_ref, s1_ref, s2_ref, s3_ref, g0_ref, g1_ref, stage_ref, ring_ref, ring_sem, in_sem, kv_sem, stage_sem):
    rows, width = xf_ref.shape
    ff = u_ref.shape[1]
    text = kbuf.shape[1]
    tn = ring_ref.shape[2]
    per = tn // 128
    nt = width // tn
    n_ff = ff // tn
    k_parts = 1
    while ff // k_parts > width or ff % k_parts:
        k_parts += 1
    kc = ff // k_parts
    part = width // CHIPS
    ring = Ring(ring_ref, ring_sem, [
        (nt, wo_ref, width, tn, 1, 0), (nt, cwq_ref, width, tn, 1, 0), (nt, cwo_ref, width, tn, 1, 0),
        (n_ff, w1_ref, width, tn, 1, 0), (nt * k_parts, w2_ref, kc, tn, k_parts, 0)])
    in_copies = [pltpu.make_async_copy(o_ref.at[d], a_ref.at[:, pl.ds(d * part, part)], in_sem) for d in range(CHIPS)]
    in_copies.append(pltpu.make_async_copy(x_hbm, b_ref, in_sem))
    for c in in_copies:
        c.start()
    ring.prime()
    load_vectors(vec_ref, (bo_ref, nw_ref, nb_ref, cgq_ref))
    BO, NW, NB, CGQ = range(4)
    mod_ref[...] = te_ref[...] + bm_ref[...]
    ss_ref[...] = jnp.zeros_like(ss_ref)
    for c in in_copies:
        c.wait()

    def vec(n, k):
        return vec_ref[n, pl.ds(k, 1), :]

    def mod(n, k):
        return mod_ref[n:n + 1, cols_of(k, 128)]

    def dots(phase, n, lhs, finish):
        def body(t, _):
            slots = [ring.wait(phase, 2 * t + i) for i in range(2)]
            for i in range(2):
                finish(2 * t + i, dot(lhs[...], ring_ref[slots[i]]))
            for i in range(2):
                ring.refill(phase, 2 * t + i)
            return 0

        lax.fori_loop(0, n // 2, body, 0)

    def o_done(i, acc):
        total = ss_ref[...]
        for g, a in enumerate(groups(acc)):
            k = i * per + g
            cols = cols_of(k, 128)
            x1 = b_ref[:, cols].astype(F32) + mod(G1, k) * (a + vec(BO, k))
            xf_ref[:, cols] = x1
            total = total + x1
        ss_ref[...] = total

    dots(0, nt, a_ref, o_done)

    def norm_to(dst, mul, add):
        def store(k, val):
            dst[:, cols_of(k, 128)] = val.astype(BF16)

        layer_norm(lambda k: xf_ref[:, cols_of(k, 128)], store, mul, add, rows, width, ss_ref, mean_ref, True)

    norm_to(b_ref, lambda k: vec(NW, k), lambda k: vec(NB, k))
    ss_ref[...] = jnp.zeros_like(ss_ref)

    def cq_done(i, acc):
        h_ref[:, cols_of(i, tn)] = acc
        add_lanes(ss_ref, rows, acc, True)

    dots(1, nt, b_ref, cq_done)
    rms_scale(ss_ref, rows, width)

    def cq_head(j, _):
        cols = cols_of(j, HEAD)
        a_ref[:, cols] = ((h_ref[:, cols] * ss_ref[...]) * vec(CGQ, j)).astype(BF16)
        return 0

    gw = kbuf.shape[2]
    n_groups = width // gw
    heads = gw // HEAD

    def kv_loads(g, slot):
        cols = cols_of(g, gw)
        return (pltpu.make_async_copy(ck_ref.at[:, cols], kbuf.at[slot], kv_sem.at[0, slot]),
                pltpu.make_async_copy(cv_ref.at[:, cols], vbuf.at[slot], kv_sem.at[1, slot]))

    for c in kv_loads(0, 0):
        c.start()
    lax.fori_loop(0, width // HEAD, cq_head, 0)
    s_refs = (s0_ref, s1_ref, s2_ref, s3_ref)

    def cross_group(g, _):
        slot = lax.rem(g, 2)
        for c in kv_loads(g, slot):
            c.wait()

        @pl.when(g + 1 < n_groups)
        def _():
            for c in kv_loads(g + 1, 1 - slot):
                c.start()

        tops = []

        def score(j):
            s = dot_nt(a_ref[:, cols_of(g * heads + j, HEAD)], kbuf[slot, :, j * HEAD:(j + 1) * HEAD])
            s_refs[j % 4][...] = s
            parts = groups(s)
            mx = parts[0]
            for p in parts[1:]:
                mx = jnp.maximum(mx, p)
            tops.append(jnp.broadcast_to(jnp.max(mx, axis=1, keepdims=True), (rows, 128)))

        def weigh(j):
            total = jnp.zeros((rows, 128), F32)
            parts = []
            for c in range(text // 128):
                p = jnp.exp2((s_refs[j % 4][:, c * 128:(c + 1) * 128] - tops[j]) * SM_C)
                total = total + p
                parts.append(p.astype(BF16))
            acc = dot(jnp.concatenate(parts, axis=1), vbuf[slot, :, j * HEAD:(j + 1) * HEAD])
            b_ref[:, cols_of(g * heads + j, HEAD)] = (acc / jnp.sum(total, axis=1, keepdims=True)).astype(BF16)

        score(0)
        for j in range(1, heads):
            score(j)
            weigh(j - 1)
        weigh(heads - 1)
        return 0

    lax.fori_loop(0, n_groups, cross_group, 0)
    ss_ref[...] = jnp.zeros_like(ss_ref)

    def co_done(i, acc):
        total = ss_ref[...]
        for g, a in enumerate(groups(acc)):
            cols = cols_of(i * per + g, 128)
            x2 = xf_ref[:, cols] + a
            xf_ref[:, cols] = x2
            total = total + x2
        ss_ref[...] = total

    dots(2, nt, b_ref, co_done)
    norm_to(a_ref, lambda k: 1.0 + mod(SC2, k), lambda k: mod(SH2, k))

    def f1_gelu(i, src, g):
        u_ref[:, cols_of(i * per + g, 128)] = jax.nn.gelu(src[:, g * 128:(g + 1) * 128], approximate=True).astype(BF16)

    def f1_dot(slot, dst, old, src):
        acc = None
        kp = width // per
        for g in range(per):
            term = dot(a_ref[:, g * kp:(g + 1) * kp], ring_ref[slot, g * kp:(g + 1) * kp, :])
            acc = term if acc is None else acc + term
            if src is not None:
                f1_gelu(old, src, g)
        dst[...] = acc

    f1_dot(ring.wait(3, 0), g0_ref, None, None)
    ring.refill(3, 0)

    def f1_pair(t, _):
        i = 2 * t + 1
        slots = [ring.wait(3, i), ring.wait(3, i + 1)]
        f1_dot(slots[0], g1_ref, i - 1, g0_ref)
        f1_dot(slots[1], g0_ref, i, g1_ref)
        ring.refill(3, i)
        ring.refill(3, i + 1)
        return 0

    lax.fori_loop(0, (n_ff - 1) // 2, f1_pair, 0)
    for g in range(per):
        f1_gelu(n_ff - 1, g0_ref, g)

    def stage_copy(i, slot):
        return pltpu.make_async_copy(stage_ref.at[slot], out_ref.at[:, cols_of(i, tn)], stage_sem.at[slot])

    def f2_tile(i, _):
        s = lax.rem(i, 2)
        slots = [ring.wait(4, i * k_parts + c) for c in range(k_parts)]

        @pl.when(i >= 2)
        def _():
            stage_copy(i, s).wait()

        acc = None
        for c in range(k_parts):
            term = dot(u_ref[:, c * kc:(c + 1) * kc], ring_ref[slots[c], 0:kc, :])
            acc = term if acc is None else acc + term
        for g, a in enumerate(groups(acc)):
            k = i * per + g
            stage_ref[s, :, g * 128:(g + 1) * 128] = (xf_ref[:, cols_of(k, 128)] + mod(G2, k) * a).astype(BF16)
        stage_copy(i, s).start()
        for c in range(k_parts):
            ring.refill(4, i * k_parts + c)
        return 0

    lax.fori_loop(0, nt, f2_tile, 0)
    for i in range(2):
        stage_copy(0, i).wait()


def tail_call(te, bm, vectors, x, o, ck, cv, wo, cwq, cwo, w1, w2, tn):
    rows, width = x.shape
    text = ck.shape[0]
    ff = w1.shape[1]
    flops = 2 * rows * width * (3 * width + 2 * ff) + 4 * rows * text * width
    assert (width // tn) % 2 == 0 and (ff // tn) % 2 == 1 and len(vectors) == 4
    return pl.pallas_call(
        tail_kernel,
        out_shape=jax.ShapeDtypeStruct((rows, width), BF16),
        in_specs=[vmem_spec()] * (2 + len(vectors)) + [any_spec()] * 9,
        out_specs=any_spec(),
        scratch_shapes=[
            pltpu.VMEM((rows, width), BF16),
            pltpu.VMEM((rows, width), BF16),
            pltpu.VMEM((rows, width), F32),
            pltpu.VMEM((rows, width), F32),
            pltpu.VMEM((rows, ff), BF16),
            pltpu.VMEM((rows, 128), F32),
            pltpu.VMEM((rows, 128), F32),
            pltpu.VMEM((len(vectors), width // 128, 128), F32),
            pltpu.VMEM(te.shape, F32),
            pltpu.VMEM((2, text, 8 * HEAD), BF16),
            pltpu.VMEM((2, text, 8 * HEAD), BF16),
            pltpu.VMEM((rows, text), F32),
            pltpu.VMEM((rows, text), F32),
            pltpu.VMEM((rows, text), F32),
            pltpu.VMEM((rows, text), F32),
            pltpu.VMEM((rows, tn), F32),
            pltpu.VMEM((rows, tn), F32),
            pltpu.VMEM((2, rows, tn), BF16),
            pltpu.VMEM((5, width, tn), BF16),
            pltpu.SemaphoreType.DMA((5,)),
            pltpu.SemaphoreType.DMA,
            pltpu.SemaphoreType.DMA((2, 2)),
            pltpu.SemaphoreType.DMA((2,)),
        ],
        compiler_params=pltpu.CompilerParams(vmem_limit_bytes=VMEM_LIMIT),
        cost_estimate=pl.CostEstimate(flops=flops, bytes_accessed=2 * width * (3 * width + 2 * ff), transcendentals=rows * ff),
        name='tail',
    )(te, bm, *vectors, x, o, ck, cv, wo, cwq, cwo, w1, w2)


def solution(mesh):
    tok_spec = P('dp', ('sp', 'uly'), None)
    batch_spec = P('dp', None, None)

    def local_block(tokens, rope_ang, t_emb, block_mod, context, attn_wq, attn_bq, attn_wk, attn_bk, attn_wv, attn_bv, attn_gq, attn_gk, attn_wo, attn_bo, norm3_w, norm3_b, cross_wq, cross_wk, cross_wv, cross_gq, cross_gk, cross_wo, ffn_w1, ffn_w2):
        x, te, bm, ctx = tokens[0], t_emb[0], block_mod[0], context[0]
        tn = min(512, x.shape[1] // CHIPS)

        def lanes(*vectors):
            return tuple(v.reshape(-1, 128) for v in vectors)

        q, k, v, ck = qkv_call(x, te, bm, rope_ang, lanes(attn_bq, attn_bk, attn_bv, attn_gq, attn_gk, cross_gk), ctx,
                               attn_wv, attn_wk, attn_wq, cross_wk, tn)
        o, cv = attend_call(q, k, v, ctx, cross_wv, tn)
        out = tail_call(te, bm, lanes(attn_bo, norm3_w, norm3_b, cross_gq), x, o, ck, cv, attn_wo, cross_wq, cross_wo, ffn_w1, ffn_w2, tn)
        return out[None]

    in_specs = (tok_spec, P(('sp', 'uly'), None), batch_spec, P(), batch_spec) + (P(),) * 20
    return jax.shard_map(local_block, mesh=mesh, in_specs=in_specs, out_specs=tok_spec, check_vma=False)
```

```python
import functools

import jax
import jax.numpy as jnp
from jax import lax
from jax.experimental import pallas as pl
from jax.experimental.pallas import tpu as pltpu
from jax.sharding import PartitionSpec as P

EPS = 1e-6
HEAD = 128
LOG2E = 1.4426950408889634
SM_C = (HEAD ** -0.5) * LOG2E
MESH = pl.DeviceIdType.MESH
CHIPS = 8
VMEM_LIMIT = 64 * 1000 * 1024
F32 = jnp.float32
BF16 = jnp.bfloat16

SH1, SC1, G1, SH2, SC2, G2 = range(6)


def dot(a, b):
    return jnp.dot(a, b, preferred_element_type=F32)


def dot_nt(a, b):
    return lax.dot_general(a, b, (((1,), (1,)), ((), ())), preferred_element_type=F32)


def my_place():
    uly = lax.axis_index('uly')
    chip = lax.axis_index('sp') * 2 + uly // 2
    return chip, lax.rem(uly, 2)


def device_at(chip, core):
    return {'sp': chip // 2, 'uly': lax.rem(chip, 2) * 2 + core}


def flip(chip, r):
    out = 0
    for bit in (1, 2, 4):
        out = out + lax.rem(chip // bit + r // bit, 2) * bit
    return out


def meet(me, core, sibling):
    barrier = pltpu.get_barrier_semaphore()
    for r in range(1, CHIPS):
        pl.semaphore_signal(barrier, inc=1, device_id=device_at(flip(me, r), core), device_id_type=MESH)
    if sibling:
        pl.semaphore_signal(barrier, inc=1, device_id=device_at(me, 1 - core), device_id_type=MESH)
    return barrier, CHIPS - 1 + int(sibling)


class Ring:
    def __init__(self, slots, sems, phases, queues=1):
        self.slots, self.sems, self.phases, self.queues = slots, sems, phases, queues
        self.depth = slots.shape[0]
        self.base = [sum(p[0] for p in phases[:i]) for i in range(len(phases) + 1)]

    def slot(self, phase, tile):
        return lax.rem(self.base[phase] + tile, self.depth)

    def copies(self, phase, tile):
        n, w_ref, k_rows, n_cols, k_parts, shift = self.phases[phase]
        slot = self.slot(phase, tile)
        cols = cols_of(lax.rem(tile // k_parts + shift, n // k_parts), n_cols)
        row0 = lax.rem(tile, k_parts) * k_rows
        quarter = k_rows // 4
        out = []
        for c in range(4):
            rows = pl.ds(pl.multiple_of(row0 + c * quarter, quarter), quarter)
            out.append(pltpu.make_async_copy(w_ref.at[rows, cols], self.slots.at[slot, pl.ds(c * quarter, quarter)], self.sems.at[slot]))
        return out

    def start(self, phase, tile):
        for n, c in enumerate(self.copies(phase, tile)):
            c.start(priority=n % self.queues)

    def prime(self):
        for i in range(self.depth):
            if i < self.phases[0][0]:
                self.start(0, i)
            else:
                self.start(1, i - self.phases[0][0])

    def wait(self, phase, tile):
        for c in self.copies(phase, tile):
            c.wait()
        return self.slot(phase, tile)

    def refill(self, phase, tile):
        n = self.phases[phase][0]
        ahead = tile + self.depth

        @pl.when(ahead < n)
        def _():
            self.start(phase, ahead)

        if phase + 1 < len(self.phases):
            @pl.when(ahead >= n)
            def _():
                self.start(phase + 1, ahead - n)


def cols_of(i, width):
    return pl.ds(pl.multiple_of(i * width, width), width)


def groups(acc):
    return [acc[:, g * 128:(g + 1) * 128] for g in range(acc.shape[1] // 128)]


def add_lanes(ref, rows, acc, squares):
    total = ref[0:rows, :]
    for part in groups(acc):
        total = total + (part * part if squares else part)
    ref[0:rows, :] = total


def lane_mean(ref, rows, width):
    return jnp.broadcast_to(jnp.sum(ref[0:rows, :], axis=1, keepdims=True) * (1.0 / width), (rows, 128))


def rms_scale(ss_ref, rows, width):
    ss_ref[0:rows, :] = lax.rsqrt(lane_mean(ss_ref, rows, width) + EPS)


def load_vectors(vec_ref, refs):
    for n, ref in enumerate(refs):
        vec_ref[n] = ref[...].astype(F32)


def layer_norm(load, store, mul, add, rows, width, sum_ref, mean_ref, have_sum):
    step = 4 if width % 512 == 0 else 1
    n = width // 128 // step

    def sums(j, _):
        total = sum_ref[0:rows, :]
        for g in range(step):
            total = total + load(j * step + g)
        sum_ref[0:rows, :] = total
        return 0

    if not have_sum:
        sum_ref[0:rows, :] = jnp.zeros((rows, 128), F32)
        lax.fori_loop(0, n, sums, 0)
    mean_ref[...] = lane_mean(sum_ref, rows, width)
    sum_ref[0:rows, :] = jnp.zeros((rows, 128), F32)

    def squares(j, _):
        total = sum_ref[0:rows, :]
        for g in range(step):
            d = load(j * step + g) - mean_ref[...]
            total = total + d * d
        sum_ref[0:rows, :] = total
        return 0

    lax.fori_loop(0, n, squares, 0)
    rms_scale(sum_ref, rows, width)

    def apply(j, _):
        for g in range(step):
            k = j * step + g
            store(k, ((load(k) - mean_ref[...]) * sum_ref[0:rows, :]) * mul(k) + add(k))
        return 0

    lax.fori_loop(0, n, apply, 0)


def qkv_kernel(x_ref, te_ref, bm_ref, ang_ref, bq_ref, bk_ref, bv_ref, gq_ref, gk_ref, cgk_ref,
               ctx_hbm, wv_ref, wk_ref, wq_ref, cwk_ref,
               q_out, k_out, v_out, ck_out,
               y_ref, h_ref, ss_ref, mean_ref, cos_ref, sin_ref, vec_ref, mod_ref, qkv_ref, ctx_ref, stage_ref, ring_ref,
               ring_sem, out_sem, ctx_sem, stage_sem, send_sem, recv_sem):
    rows, width = x_ref.shape
    text = ctx_ref.shape[0]
    tn = ring_ref.shape[2]
    per = tn // 128
    nt = width // tn
    part = width // CHIPS
    me, core = my_place()
    barrier, n_signals = meet(me, core, False)
    far = (CHIPS // 2) * (1 - me // (CHIPS // 2))
    shift = far * part // tn
    ring = Ring(ring_ref, ring_sem, [(nt, w, width, tn, 1, sh) for w, sh in ((wv_ref, shift), (wk_ref, 0), (wq_ref, 0), (cwk_ref, 0))])
    ring.prime()
    ctx_copy = pltpu.make_async_copy(ctx_hbm, ctx_ref, ctx_sem)
    ctx_copy.start()
    load_vectors(vec_ref, (bq_ref, bk_ref, bv_ref, gq_ref, gk_ref, cgk_ref))
    BQ, BK, BV, GQ, GK, CGK = range(6)
    mod_ref[...] = te_ref[...] + bm_ref[...]

    def vec(n, k):
        return vec_ref[n, pl.ds(k, 1), :]

    def store_y(k, val):
        y_ref[:, cols_of(k, 128)] = val.astype(BF16)

    layer_norm(lambda k: x_ref[:, cols_of(k, 128)].astype(F32), store_y,
               lambda k: 1.0 + mod_ref[SC1, pl.ds(k, 1), :], lambda k: mod_ref[SH1, pl.ds(k, 1), :],
               rows, width, ss_ref, mean_ref, False)
    pl.semaphore_wait(barrier, n_signals)

    def remote(n, dst, r):
        to = flip(me, r)
        return pltpu.make_async_remote_copy(
            src_ref=qkv_ref.at[n, :, cols_of(to, part)], dst_ref=dst.at[cols_of(me, rows)],
            send_sem=send_sem.at[n, r], recv_sem=recv_sem.at[n, r], device_id=device_at(to, core), device_id_type=MESH)

    def local(n, dst):
        return pltpu.make_async_copy(qkv_ref.at[n, :, cols_of(me, part)], dst.at[cols_of(me, rows)], out_sem.at[n])

    def q_copies():
        return [pltpu.make_async_copy(qkv_ref.at[2, :, pl.ds(d * part, part)], q_out.at[d], out_sem.at[2]) for d in range(CHIPS)]

    def v_tile(i, _):
        slot = ring.wait(0, i)
        for j in range(CHIPS // 2):
            @pl.when(i == -(-part * (j + 1) // tn))
            def _():
                remote(0, v_out, flip(me, far + j)).start()

        ct = lax.rem(i + shift, nt)
        for g, a in enumerate(groups(dot(y_ref[...], ring_ref[slot]))):
            k = ct * per + g
            qkv_ref[0, :, cols_of(k, 128)] = (a + vec(BV, k)).astype(BF16)
        ring.refill(0, i)
        return 0

    lax.fori_loop(0, nt, v_tile, 0)

    def v_rest():
        for r in range(1, CHIPS // 2):
            remote(0, v_out, r).start()
        local(0, v_out).start()
        lane = lax.broadcasted_iota(jnp.int32, (rows, HEAD), 1)
        ang = jnp.concatenate([ang_ref[...], ang_ref[...]], axis=1)
        spread = jnp.take_along_axis(ang, lane // 2, axis=1)
        cos_ref[...] = jnp.cos(spread)
        sin_ref[...] = jnp.where(lax.rem(lane, 2) == 0, -1.0, 1.0) * jnp.sin(spread)

    def k_all():
        for r in range(CHIPS - 1, 0, -1):
            remote(1, k_out, r).start()
        local(1, k_out).start()

    def q_all():
        for c in q_copies():
            c.start()
        ctx_copy.wait()

    def normed_phase(phase, n, b, gain, send_last):
        ss_ref[0:rows, :] = jnp.zeros((rows, 128), F32)

        def tile(i, _):
            slot = ring.wait(phase, i)
            pl.when(i == 0)(send_last)
            total = ss_ref[0:rows, :]
            for g, a in enumerate(groups(dot(y_ref[...], ring_ref[slot]))):
                k = i * per + g
                a = a + vec(b, k)
                h_ref[0:rows, cols_of(k, 128)] = a
                total = total + a * a
            ss_ref[0:rows, :] = total
            ring.refill(phase, i)
            return 0

        lax.fori_loop(0, nt, tile, 0)
        rms_scale(ss_ref, rows, width)
        even = lax.rem(lax.broadcasted_iota(jnp.int32, (rows, HEAD), 1), 2) == 0

        def head(j, _):
            cols = cols_of(j, HEAD)
            x = (h_ref[0:rows, cols] * ss_ref[0:rows, :]) * vec(gain, j)
            other = jnp.where(even, pltpu.roll(x, HEAD - 1, 1), pltpu.roll(x, 1, 1))
            qkv_ref[n, :, cols] = (x * cos_ref[...] + other * sin_ref[...]).astype(BF16)
            return 0

        lax.fori_loop(0, width // HEAD, head, 0)

    normed_phase(1, 1, BK, GK, v_rest)
    normed_phase(2, 2, BQ, GQ, k_all)

    def stage_copy(i, slot):
        return pltpu.make_async_copy(stage_ref.at[slot], ck_out.at[:, cols_of(i, tn)], stage_sem.at[slot])

    ss_ref[...] = jnp.zeros_like(ss_ref)

    def ck_tile(i, _):
        slot = ring.wait(3, i)
        pl.when(i == 0)(q_all)
        acc = dot(ctx_ref[...], ring_ref[slot])
        h_ref[:, cols_of(i, tn)] = acc
        add_lanes(ss_ref, text, acc, True)
        ring.refill(3, i)
        return 0

    lax.fori_loop(0, nt, ck_tile, 0)
    rms_scale(ss_ref, text, width)

    def ck_norm(i, _):
        s = lax.rem(i, 2)

        @pl.when(i >= 2)
        def _():
            stage_copy(i, s).wait()

        for j in range(per):
            k = i * per + j
            stage_ref[s, :, j * HEAD:(j + 1) * HEAD] = ((h_ref[:, cols_of(k, 128)] * ss_ref[...]) * vec(CGK, k)).astype(BF16)
        stage_copy(i, s).start()
        return 0

    lax.fori_loop(0, nt, ck_norm, 0)
    for i in range(2):
        stage_copy(0, i).wait()
    for c in q_copies():
        c.wait()
    for n, dst in ((0, v_out), (1, k_out)):
        local(n, dst).wait()
        for r in range(1, CHIPS):
            remote(n, dst, r).wait()


def any_spec():
    return pl.BlockSpec(memory_space=pl.ANY)


def vmem_spec():
    return pl.BlockSpec(memory_space=pltpu.VMEM)


def qkv_call(x, te, bm, ang, vectors, ctx, wv, wk, wq, cwk, tn):
    rows, width = x.shape
    text = ctx.shape[0]
    part = width // CHIPS
    split = jax.ShapeDtypeStruct((CHIPS, rows, part), BF16)
    gathered = jax.ShapeDtypeStruct((CHIPS * rows, part), BF16)
    flops = 2 * width * width * (3 * rows + text)
    return pl.pallas_call(
        qkv_kernel,
        out_shape=(split, gathered, gathered, jax.ShapeDtypeStruct((text, width), BF16)),
        in_specs=[vmem_spec()] * (4 + len(vectors)) + [any_spec()] * 5,
        out_specs=[any_spec()] * 4,
        scratch_shapes=[
            pltpu.VMEM((rows, width), BF16),
            pltpu.VMEM((text, width), F32),
            pltpu.VMEM((text, 128), F32),
            pltpu.VMEM((rows, 128), F32),
            pltpu.VMEM((rows, 128), F32),
            pltpu.VMEM((rows, 128), F32),
            pltpu.VMEM((len(vectors), width // 128, 128), F32),
            pltpu.VMEM(te.shape, F32),
            pltpu.VMEM((3, rows, width), BF16),
            pltpu.VMEM((text, width), BF16),
            pltpu.VMEM((2, text, tn), BF16),
            pltpu.VMEM((3, width, tn), BF16),
            pltpu.SemaphoreType.DMA((3,)),
            pltpu.SemaphoreType.DMA((3,)),
            pltpu.SemaphoreType.DMA,
            pltpu.SemaphoreType.DMA((2,)),
            pltpu.SemaphoreType.DMA((2, CHIPS)),
            pltpu.SemaphoreType.DMA((2, CHIPS)),
        ],
        compiler_params=pltpu.CompilerParams(vmem_limit_bytes=VMEM_LIMIT, collective_id=0, has_side_effects=True),
        cost_estimate=pl.CostEstimate(flops=flops, bytes_accessed=8 * width * width, transcendentals=0),
        name='qkv',
    )(x, te, bm, ang, *vectors, ctx, wv, wk, wq, cwk)


def attend_kernel(te_ref, bm_ref, bo_ref, q_ref, k_ref, v_ref, ctx_hbm, cwv_ref, x_hbm, wo_ref, x1_out, cv_out,
                  kbuf, vbuf, qbuf, obuf, s0_ref, s1_ref, mx0_ref, mx1_ref, ctx_ref, stage_ref, ring_ref, acc_ref, wo_ring, row_ref,
                  own_sem, pair_send, pair_recv, q_send, q_recv, o_send, o_recv, ctx_sem, stage_sem, ring_sem, wo_sem):
    n_heads, keys, _ = kbuf.shape
    half = keys // 2
    rows = qbuf.shape[1]
    blocks = CHIPS * n_heads
    kb = 512 if keys % 512 == 0 else keys
    n_kb = keys // kb
    me, core = my_place()
    barrier, n_signals = meet(me, core, True)

    def own(h):
        return [pltpu.make_async_copy(src.at[:, cols_of(h, HEAD)], dst.at[h, 0:half, :], own_sem.at[n, h])
                for n, (src, dst) in enumerate(((k_ref, kbuf), (v_ref, vbuf)))]

    def pair(h):
        return [pltpu.make_async_remote_copy(
            src_ref=src.at[:, cols_of(h, HEAD)], dst_ref=dst.at[h, pl.ds(half, half), :],
            send_sem=pair_send.at[n, h], recv_sem=pair_recv.at[n, h], device_id=device_at(me, 1 - core), device_id_type=MESH)
            for n, (src, dst) in enumerate(((k_ref, kbuf), (v_ref, vbuf)))]

    def q_local():
        return pltpu.make_async_copy(q_ref.at[me], qbuf.at[0], q_recv.at[0])

    def q_remote(r):
        to = flip(me, r)
        return pltpu.make_async_remote_copy(
            src_ref=q_ref.at[to], dst_ref=qbuf.at[r], send_sem=q_send.at[r], recv_sem=q_recv.at[r],
            device_id=device_at(to, core), device_id_type=MESH)

    def o_remote(r, h):
        cols = cols_of(h, HEAD)
        return pltpu.make_async_remote_copy(
            src_ref=qbuf.at[r, :, cols], dst_ref=obuf.at[r, :, cols], send_sem=o_send.at[r, h], recv_sem=o_recv.at[r, h],
            device_id=device_at(flip(me, r), core), device_id_type=MESH)

    q_local().start()
    for h in range(n_heads):
        for c in own(h):
            c.start()
    pl.semaphore_wait(barrier, n_signals)
    for c in pair(0):
        c.start()
    for r in range(1, CHIPS):
        q_remote(r).start()
    for h in range(1, n_heads):
        for c in pair(h):
            c.start()
    tn = ring_ref.shape[2]
    nt = ring_ref.shape[1] // tn
    ring = Ring(ring_ref, ring_sem, [(nt, cwv_ref, ring_ref.shape[1], tn, 1, 0)])
    ring.prime()
    ctx_copy = pltpu.make_async_copy(ctx_hbm, ctx_ref, ctx_sem)
    ctx_copy.start()

    def stage_copy(i, slot):
        return pltpu.make_async_copy(stage_ref.at[slot], cv_out.at[:, cols_of(i, tn)], stage_sem.at[slot])

    def wo_copy(r, side):
        return pltpu.make_async_copy(wo_ref.at[cols_of(flip(me, r), wo_ring.shape[1]), pl.ds(side * wo_ring.shape[2], wo_ring.shape[2])],
                                     wo_ring.at[side], wo_sem.at[side])

    for side in range(2):
        wo_copy(0, side).start()

    def cv_tile(i):
        slot = ring.wait(0, i)
        s = lax.rem(i, 2)

        @pl.when(i == 0)
        def _():
            ctx_copy.wait()

        @pl.when(i >= 2)
        def _():
            stage_copy(i, s).wait()

        stage_ref[s] = dot(ctx_ref[...], ring_ref[slot]).astype(BF16)
        stage_copy(i, s).start()
        ring.refill(0, i)

    def send_output(b):
        r, h = b // n_heads, lax.rem(b, n_heads)

        @pl.when(r > 0)
        def _():
            o_remote(r, h).start()

    def step(i, now, before):
        s_now, mx_now = now
        cur = jnp.minimum(i, blocks - 1)
        r, h = cur // n_heads, lax.rem(cur, n_heads)

        @pl.when(i < n_heads)
        def _():
            for c in own(h):
                c.wait()
            for c in pair(h):
                c.wait_recv()

        @pl.when(i == 0)
        def _():
            q_local().wait()

        @pl.when((i > 0) & (i < blocks) & (h == 0))
        def _():
            q_remote(r).wait_recv()

        if before is not None:
            @pl.when(i >= 2)
            def _():
                send_output(i - 2)

            s_old, mx_old = before
            old_r, old_h = (i - 1) // n_heads, lax.rem(i - 1, n_heads)
            total = jnp.zeros((rows, 128), F32)
            acc = jnp.zeros((rows, HEAD), F32)
        q = qbuf[r, :, cols_of(h, HEAD)]
        mx = None
        for j in range(n_kb):
            s = dot_nt(q, kbuf[h, j * kb:(j + 1) * kb, :])
            s_now[:, j * kb:(j + 1) * kb] = s
            for g in range(kb // 128):
                sg = s[:, g * 128:(g + 1) * 128]
                mx = sg if mx is None else jnp.maximum(mx, sg)
            if before is not None:
                parts = []
                for g in range(kb // 128):
                    c0 = j * kb + g * 128
                    p = jnp.exp2((s_old[:, c0:c0 + 128] - mx_old[...]) * SM_C)
                    total = total + p
                    parts.append(p.astype(BF16))
                acc = acc + dot(jnp.concatenate(parts, axis=1), vbuf[old_h, j * kb:(j + 1) * kb, :])
        mx_now[...] = jnp.broadcast_to(jnp.max(mx, axis=1, keepdims=True), (rows, 128))
        if before is not None:
            qbuf[old_r, :, cols_of(old_h, HEAD)] = (acc / jnp.sum(total, axis=1, keepdims=True)).astype(BF16)

    bufs = ((s0_ref, mx0_ref), (s1_ref, mx1_ref))
    step(jnp.int32(0), bufs[0], None)

    def pair_of_steps(t, _):
        step(2 * t + 1, bufs[1], bufs[0])
        step(2 * t + 2, bufs[0], bufs[1])

        @pl.when((lax.rem(t, every) == 0) & (t < nt * every))
        def _():
            cv_tile(t // every)

        return 0

    every = blocks // 2 // nt
    lax.fori_loop(0, blocks // 2, pair_of_steps, 0)
    send_output(jnp.int32(blocks - 1))
    for i in range(2):
        stage_copy(0, i).wait()
    width = acc_ref.shape[1]
    part = qbuf.shape[2]
    half_n = width // 2
    x_copy = pltpu.make_async_copy(x_hbm, ctx_ref.at[0:rows], ctx_sem)
    x_copy.start()
    row_ref[0] = te_ref[G1] + bm_ref[G1]
    row_ref[1] = bo_ref[...].astype(F32)

    def project(r, lhs, side, finish):
        wo_copy(r, side).wait()
        for n in range(half_n // tn):
            cols = pl.ds(side * half_n + n * tn, tn)
            finish(cols, side * half_n + n * tn, dot(lhs[...], wo_ring[side, :, n * tn:(n + 1) * tn]))

    def first(cols, c0, prod):
        acc_ref[:, cols] = prod

    def middle(cols, c0, prod):
        acc_ref[:, cols] = acc_ref[:, cols] + prod

    def last(cols, c0, prod):
        for g, p in enumerate(groups(prod)):
            k = c0 // 128 + g
            gc = slice(c0 + g * 128, c0 + (g + 1) * 128)
            acc_ref[:, gc] = ctx_ref[0:rows, gc].astype(F32) + row_ref[0, k:k + 1, :] * (acc_ref[:, gc] + p + row_ref[1, k:k + 1, :])

    def arrived(r):
        for h in range(n_heads):
            o_remote(r, h).wait_recv()

    def x1_copy(side):
        cols = pl.ds(side * half_n, half_n)
        return pltpu.make_async_copy(acc_ref.at[:, cols], x1_out.at[:, cols], stage_sem.at[side])

    for side in range(2):
        project(0, qbuf.at[0], side, first)
        wo_copy(1, side).start()

    def chunk(r, _):
        arrived(r)
        for side in range(2):
            project(r, obuf.at[r], side, middle)
            wo_copy(r + 1, side).start()
        return 0

    lax.fori_loop(1, CHIPS - 1, chunk, 0)
    x_copy.wait()
    arrived(CHIPS - 1)
    project(CHIPS - 1, obuf.at[CHIPS - 1], 0, last)
    project(CHIPS - 1, obuf.at[CHIPS - 1], 1, last)
    x1_copy(0).start()
    for h in range(n_heads):
        for c in pair(h):
            c.wait_send()

    def drain(r, _):
        q_remote(r).wait_send()
        for h in range(n_heads):
            o_remote(r, h).wait_send()
        return 0

    lax.fori_loop(1, CHIPS, drain, 0)
    x1_copy(1).start()
    for side in range(2):
        x1_copy(side).wait()


def attend_call(te, bm, bo, q, k, v, ctx, cwv, x, wo, tn):
    _, rows, part = q.shape
    half = k.shape[0]
    n_heads = part // HEAD
    text, width = ctx.shape
    flops = 8 * half * half * part + 2 * (text + rows) * width * width
    return pl.pallas_call(
        attend_kernel,
        out_shape=(jax.ShapeDtypeStruct((rows, width), F32), jax.ShapeDtypeStruct((text, width), BF16)),
        in_specs=[vmem_spec()] * 3 + [any_spec()] * 7,
        out_specs=[any_spec()] * 2,
        scratch_shapes=[
            pltpu.VMEM((n_heads, 2 * half, HEAD), BF16),
            pltpu.VMEM((n_heads, 2 * half, HEAD), BF16),
            pltpu.VMEM((CHIPS, rows, part), BF16),
            pltpu.VMEM((CHIPS, rows, part), BF16),
            pltpu.VMEM((rows, 2 * half), F32),
            pltpu.VMEM((rows, 2 * half), F32),
            pltpu.VMEM((rows, 128), F32),
            pltpu.VMEM((rows, 128), F32),
            pltpu.VMEM((text, width), BF16),
            pltpu.VMEM((2, text, tn), BF16),
            pltpu.VMEM((2, width, tn), BF16),
            pltpu.VMEM((rows, width), F32),
            pltpu.VMEM((2, part, width // 2), BF16),
            pltpu.VMEM((2, width // 128, 128), F32),
            pltpu.SemaphoreType.DMA((2, n_heads)),
            pltpu.SemaphoreType.DMA((2, n_heads)),
            pltpu.SemaphoreType.DMA((2, n_heads)),
            pltpu.SemaphoreType.DMA((CHIPS,)),
            pltpu.SemaphoreType.DMA((CHIPS,)),
            pltpu.SemaphoreType.DMA((CHIPS, n_heads)),
            pltpu.SemaphoreType.DMA((CHIPS, n_heads)),
            pltpu.SemaphoreType.DMA,
            pltpu.SemaphoreType.DMA((2,)),
            pltpu.SemaphoreType.DMA((2,)),
            pltpu.SemaphoreType.DMA((2,)),
        ],
        compiler_params=pltpu.CompilerParams(vmem_limit_bytes=VMEM_LIMIT, collective_id=1, has_side_effects=True),
        cost_estimate=pl.CostEstimate(flops=flops, bytes_accessed=8 * half * part + 4 * width * width, transcendentals=2 * half * half * n_heads),
        name='attend',
    )(te, bm, bo, q, k, v, ctx, cwv, x, wo)


def tail_kernel(te_ref, bm_ref, nw_ref, nb_ref, cgq_ref, x1_ref, ck_ref, cv_ref, cwq_ref, cwo_ref, w1_ref, w2_ref,
                out_ref, a_ref, b_ref, xf_ref, h_ref, u_ref, ss_ref, mean_ref, vec_ref, mod_ref, kbuf, vbuf,
                s0_ref, s1_ref, s2_ref, s3_ref, g0_ref, g1_ref, stage_ref, ring_ref, ring_sem, in_sem, kv_sem, stage_sem):
    rows, width = xf_ref.shape
    ff = u_ref.shape[1]
    text = kbuf.shape[1]
    tn = ring_ref.shape[2]
    per = tn // 128
    nt = width // tn
    n_ff = ff // tn
    k_parts = 1
    while ff // k_parts > width or ff % k_parts:
        k_parts += 1
    kc = ff // k_parts
    ring = Ring(ring_ref, ring_sem, [
        (nt, cwq_ref, width, tn, 1, 0), (nt, cwo_ref, width, tn, 1, 0),
        (n_ff, w1_ref, width, tn, 1, 0), (nt * k_parts, w2_ref, kc, tn, k_parts, 0)], 2)
    x1_copy = pltpu.make_async_copy(x1_ref, xf_ref, in_sem)
    x1_copy.start()
    ring.prime()
    load_vectors(vec_ref, (nw_ref, nb_ref, cgq_ref))
    NW, NB, CGQ = range(3)
    mod_ref[...] = te_ref[...] + bm_ref[...]
    x1_copy.wait()

    def vec(n, k):
        return vec_ref[n, pl.ds(k, 1), :]

    def mod(n, k):
        return mod_ref[n, pl.ds(k, 1), :]

    def dots(phase, n, lhs, finish):
        def body(t, _):
            slots = [ring.wait(phase, 2 * t + i) for i in range(2)]
            for i in range(2):
                finish(2 * t + i, dot(lhs[...], ring_ref[slots[i]]))
            for i in range(2):
                ring.refill(phase, 2 * t + i)
            return 0

        lax.fori_loop(0, n // 2, body, 0)

    def norm_to(dst, mul, add, have_sum):
        def store(k, val):
            dst[:, cols_of(k, 128)] = val.astype(BF16)

        layer_norm(lambda k: xf_ref[:, cols_of(k, 128)], store, mul, add, rows, width, ss_ref, mean_ref, have_sum)

    norm_to(b_ref, lambda k: vec(NW, k), lambda k: vec(NB, k), False)
    ss_ref[...] = jnp.zeros_like(ss_ref)

    def cq_done(i, acc):
        h_ref[:, cols_of(i, tn)] = acc
        add_lanes(ss_ref, rows, acc, True)

    dots(0, nt, b_ref, cq_done)
    rms_scale(ss_ref, rows, width)

    def cq_head(j, _):
        cols = cols_of(j, HEAD)
        a_ref[:, cols] = ((h_ref[:, cols] * ss_ref[...]) * vec(CGQ, j)).astype(BF16)
        return 0

    gw = kbuf.shape[2]
    n_groups = width // gw
    heads = gw // HEAD

    def kv_loads(g, slot):
        cols = cols_of(g, gw)
        return (pltpu.make_async_copy(ck_ref.at[:, cols], kbuf.at[slot], kv_sem.at[0, slot]),
                pltpu.make_async_copy(cv_ref.at[:, cols], vbuf.at[slot], kv_sem.at[1, slot]))

    for c in kv_loads(0, 0):
        c.start()
    lax.fori_loop(0, width // HEAD, cq_head, 0)
    s_refs = (s0_ref, s1_ref, s2_ref, s3_ref)

    def cross_group(g, _):
        slot = lax.rem(g, 2)
        for c in kv_loads(g, slot):
            c.wait()

        @pl.when(g + 1 < n_groups)
        def _():
            for c in kv_loads(g + 1, 1 - slot):
                c.start()

        tops = []

        def score(j):
            s = dot_nt(a_ref[:, cols_of(g * heads + j, HEAD)], kbuf[slot, :, j * HEAD:(j + 1) * HEAD])
            s_refs[j % 4][...] = s
            parts = groups(s)
            mx = parts[0]
            for p in parts[1:]:
                mx = jnp.maximum(mx, p)
            tops.append(jnp.broadcast_to(jnp.max(mx, axis=1, keepdims=True), (rows, 128)))

        def weigh(j):
            total = jnp.zeros((rows, 128), F32)
            parts = []
            for c in range(text // 128):
                p = jnp.exp2((s_refs[j % 4][:, c * 128:(c + 1) * 128] - tops[j]) * SM_C)
                total = total + p
                parts.append(p.astype(BF16))
            acc = dot(jnp.concatenate(parts, axis=1), vbuf[slot, :, j * HEAD:(j + 1) * HEAD])
            b_ref[:, cols_of(g * heads + j, HEAD)] = (acc / jnp.sum(total, axis=1, keepdims=True)).astype(BF16)

        score(0)
        for j in range(1, heads):
            score(j)
            weigh(j - 1)
        weigh(heads - 1)
        return 0

    lax.fori_loop(0, n_groups, cross_group, 0)
    ss_ref[...] = jnp.zeros_like(ss_ref)

    def co_done(i, acc):
        total = ss_ref[...]
        for g, a in enumerate(groups(acc)):
            cols = cols_of(i * per + g, 128)
            x2 = xf_ref[:, cols] + a
            xf_ref[:, cols] = x2
            total = total + x2
        ss_ref[...] = total

    dots(1, nt, b_ref, co_done)
    norm_to(a_ref, lambda k: 1.0 + mod(SC2, k), lambda k: mod(SH2, k), True)

    def f1_gelu(i, src, g):
        u_ref[:, cols_of(i * per + g, 128)] = jax.nn.gelu(src[:, g * 128:(g + 1) * 128], approximate=True).astype(BF16)

    def f1_dot(slot, dst, old, src):
        acc = None
        kp = width // per
        for g in range(per):
            term = dot(a_ref[:, g * kp:(g + 1) * kp], ring_ref[slot, g * kp:(g + 1) * kp, :])
            acc = term if acc is None else acc + term
            if src is not None:
                f1_gelu(old, src, g)
        dst[...] = acc

    f1_dot(ring.wait(2, 0), g0_ref, None, None)
    ring.refill(2, 0)

    def f1_pair(t, _):
        i = 2 * t + 1
        slots = [ring.wait(2, i), ring.wait(2, i + 1)]
        f1_dot(slots[0], g1_ref, i - 1, g0_ref)
        f1_dot(slots[1], g0_ref, i, g1_ref)
        ring.refill(2, i)
        ring.refill(2, i + 1)
        return 0

    lax.fori_loop(0, (n_ff - 1) // 2, f1_pair, 0)
    for g in range(per):
        f1_gelu(n_ff - 1, g0_ref, g)

    def stage_copy(i, slot):
        return pltpu.make_async_copy(stage_ref.at[slot], out_ref.at[:, cols_of(i, tn)], stage_sem.at[slot])

    def f2_tile(i, _):
        s = lax.rem(i, 2)
        slots = [ring.wait(3, i * k_parts + c) for c in range(k_parts)]

        @pl.when(i >= 2)
        def _():
            stage_copy(i, s).wait()

        acc = None
        for c in range(k_parts):
            term = dot(u_ref[:, c * kc:(c + 1) * kc], ring_ref[slots[c], 0:kc, :])
            acc = term if acc is None else acc + term
        for g, a in enumerate(groups(acc)):
            k = i * per + g
            stage_ref[s, :, g * 128:(g + 1) * 128] = (xf_ref[:, cols_of(k, 128)] + mod(G2, k) * a).astype(BF16)
        stage_copy(i, s).start()
        for c in range(k_parts):
            ring.refill(3, i * k_parts + c)
        return 0

    lax.fori_loop(0, nt, f2_tile, 0)
    for i in range(2):
        stage_copy(0, i).wait()


def tail_call(te, bm, vectors, x1, ck, cv, cwq, cwo, w1, w2, tn):
    rows, width = x1.shape
    text = ck.shape[0]
    ff = w1.shape[1]
    flops = 2 * rows * width * (2 * width + 2 * ff) + 4 * rows * text * width
    assert (width // tn) % 2 == 0 and (ff // tn) % 2 == 1 and len(vectors) == 3
    return pl.pallas_call(
        tail_kernel,
        out_shape=jax.ShapeDtypeStruct((rows, width), BF16),
        in_specs=[vmem_spec()] * (2 + len(vectors)) + [any_spec()] * 7,
        out_specs=any_spec(),
        scratch_shapes=[
            pltpu.VMEM((rows, width), BF16),
            pltpu.VMEM((rows, width), BF16),
            pltpu.VMEM((rows, width), F32),
            pltpu.VMEM((rows, width), F32),
            pltpu.VMEM((rows, ff), BF16),
            pltpu.VMEM((rows, 128), F32),
            pltpu.VMEM((rows, 128), F32),
            pltpu.VMEM((len(vectors), width // 128, 128), F32),
            pltpu.VMEM(te.shape, F32),
            pltpu.VMEM((2, text, 8 * HEAD), BF16),
            pltpu.VMEM((2, text, 8 * HEAD), BF16),
            pltpu.VMEM((rows, text), F32),
            pltpu.VMEM((rows, text), F32),
            pltpu.VMEM((rows, text), F32),
            pltpu.VMEM((rows, text), F32),
            pltpu.VMEM((rows, tn), F32),
            pltpu.VMEM((rows, tn), F32),
            pltpu.VMEM((2, rows, tn), BF16),
            pltpu.VMEM((5, width, tn), BF16),
            pltpu.SemaphoreType.DMA((5,)),
            pltpu.SemaphoreType.DMA,
            pltpu.SemaphoreType.DMA((2, 2)),
            pltpu.SemaphoreType.DMA((2,)),
        ],
        compiler_params=pltpu.CompilerParams(vmem_limit_bytes=VMEM_LIMIT),
        cost_estimate=pl.CostEstimate(flops=flops, bytes_accessed=2 * width * (2 * width + 2 * ff), transcendentals=rows * ff),
        name='tail',
    )(te, bm, *vectors, x1, ck, cv, cwq, cwo, w1, w2)


def solution(mesh):
    tok_spec = P('dp', ('sp', 'uly'), None)
    batch_spec = P('dp', None, None)

    def local_block(tokens, rope_ang, t_emb, block_mod, context, attn_wq, attn_bq, attn_wk, attn_bk, attn_wv, attn_bv, attn_gq, attn_gk, attn_wo, attn_bo, norm3_w, norm3_b, cross_wq, cross_wk, cross_wv, cross_gq, cross_gk, cross_wo, ffn_w1, ffn_w2):
        x, ctx = tokens[0], context[0]
        te, bm = (m.reshape(6, -1, 128) for m in (t_emb, block_mod))
        tn = min(512, x.shape[1] // CHIPS)

        def lanes(*vectors):
            return tuple(v.reshape(-1, 128) for v in vectors)

        q, k, v, ck = qkv_call(x, te, bm, rope_ang, lanes(attn_bq, attn_bk, attn_bv, attn_gq, attn_gk, cross_gk), ctx,
                               attn_wv, attn_wk, attn_wq, cross_wk, tn)
        x1, cv = attend_call(te, bm, *lanes(attn_bo), q, k, v, ctx, cross_wv, x, attn_wo, tn)
        out = tail_call(te, bm, lanes(norm3_w, norm3_b, cross_gq), x1, ck, cv, cross_wq, cross_wo, ffn_w1, ffn_w2, tn)
        return out[None]

    in_specs = (tok_spec, P(('sp', 'uly'), None), batch_spec, P(), batch_spec) + (P(),) * 20
    return jax.shard_map(local_block, mesh=mesh, in_specs=in_specs, out_specs=tok_spec, check_vma=False)
```

```python
import functools

import jax
import jax.numpy as jnp
from jax import lax
from jax.experimental import pallas as pl
from jax.experimental.pallas import tpu as pltpu
from jax.sharding import PartitionSpec as P

EPS = 1e-6
HEAD = 128
LOG2E = 1.4426950408889634
SM_C = (HEAD ** -0.5) * LOG2E
MESH = pl.DeviceIdType.MESH
CHIPS = 8
VMEM_LIMIT = 64 * 1000 * 1024
F32 = jnp.float32
BF16 = jnp.bfloat16

SH1, SC1, G1, SH2, SC2, G2 = range(6)


def dot(a, b):
    return jnp.dot(a, b, preferred_element_type=F32)


def dot_nt(a, b):
    return lax.dot_general(a, b, (((1,), (1,)), ((), ())), preferred_element_type=F32)


def my_place():
    uly = lax.axis_index('uly')
    chip = lax.axis_index('sp') * 2 + uly // 2
    return chip, lax.rem(uly, 2)


def device_at(chip, core):
    return {'sp': chip // 2, 'uly': lax.rem(chip, 2) * 2 + core}


def flip(chip, r):
    out = 0
    for bit in (1, 2, 4):
        out = out + lax.rem(chip // bit + r // bit, 2) * bit
    return out


def meet(me, core, sibling):
    barrier = pltpu.get_barrier_semaphore()
    for r in range(1, CHIPS):
        pl.semaphore_signal(barrier, inc=1, device_id=device_at(flip(me, r), core), device_id_type=MESH)
    if sibling:
        pl.semaphore_signal(barrier, inc=1, device_id=device_at(me, 1 - core), device_id_type=MESH)
    return barrier, CHIPS - 1 + int(sibling)


class Ring:
    def __init__(self, slots, sems, phases):
        self.slots, self.sems, self.phases = slots, sems, phases
        self.depth = slots.shape[0]
        self.base = [sum(p[0] for p in phases[:i]) for i in range(len(phases) + 1)]

    def slot(self, phase, tile):
        return lax.rem(self.base[phase] + tile, self.depth)

    def copies(self, phase, tile):
        n, w_ref, k_rows, n_cols, k_parts, shift, col0 = self.phases[phase]
        slot = self.slot(phase, tile)
        cols = cols_of(col0 + lax.rem(tile // k_parts + shift, n // k_parts), n_cols)
        row0 = lax.rem(tile, k_parts) * k_rows
        quarter = k_rows // 4
        out = []
        for c in range(4):
            rows = pl.ds(pl.multiple_of(row0 + c * quarter, quarter), quarter)
            out.append(pltpu.make_async_copy(w_ref.at[rows, cols], self.slots.at[slot, pl.ds(c * quarter, quarter)], self.sems.at[slot]))
        return out

    def start(self, phase, tile):
        for c in self.copies(phase, tile):
            c.start()

    def prime(self):
        for i in range(self.depth):
            if i < self.phases[0][0]:
                self.start(0, i)
            else:
                self.start(1, i - self.phases[0][0])

    def wait(self, phase, tile):
        for c in self.copies(phase, tile):
            c.wait()
        return self.slot(phase, tile)

    def refill(self, phase, tile):
        n = self.phases[phase][0]
        ahead = tile + self.depth

        @pl.when(ahead < n)
        def _():
            self.start(phase, ahead)

        if phase + 1 < len(self.phases):
            @pl.when(ahead >= n)
            def _():
                self.start(phase + 1, ahead - n)


def cols_of(i, width):
    return pl.ds(pl.multiple_of(i * width, width), width)


def groups(acc):
    return [acc[:, g * 128:(g + 1) * 128] for g in range(acc.shape[1] // 128)]


def add_lanes(ref, rows, acc, squares):
    total = ref[0:rows, :]
    for part in groups(acc):
        total = total + (part * part if squares else part)
    ref[0:rows, :] = total


def lane_mean(ref, rows, width):
    return jnp.broadcast_to(jnp.sum(ref[0:rows, :], axis=1, keepdims=True) * (1.0 / width), (rows, 128))


def rms_scale(ss_ref, rows, width):
    ss_ref[0:rows, :] = lax.rsqrt(lane_mean(ss_ref, rows, width) + EPS)


def load_vectors(vec_ref, refs):
    for n, ref in enumerate(refs):
        vec_ref[n] = ref[...].astype(F32)


def layer_norm(load, store, mul, add, rows, width, sum_ref, mean_ref, have_sum):
    step = 4 if width % 512 == 0 else 1
    n = width // 128 // step

    def sums(j, _):
        total = sum_ref[0:rows, :]
        for g in range(step):
            total = total + load(j * step + g)
        sum_ref[0:rows, :] = total
        return 0

    if not have_sum:
        sum_ref[0:rows, :] = jnp.zeros((rows, 128), F32)
        lax.fori_loop(0, n, sums, 0)
    mean_ref[...] = lane_mean(sum_ref, rows, width)
    sum_ref[0:rows, :] = jnp.zeros((rows, 128), F32)

    def squares(j, _):
        total = sum_ref[0:rows, :]
        for g in range(step):
            d = load(j * step + g) - mean_ref[...]
            total = total + d * d
        sum_ref[0:rows, :] = total
        return 0

    lax.fori_loop(0, n, squares, 0)
    rms_scale(sum_ref, rows, width)

    def apply(j, _):
        for g in range(step):
            k = j * step + g
            store(k, ((load(k) - mean_ref[...]) * sum_ref[0:rows, :]) * mul(k) + add(k))
        return 0

    lax.fori_loop(0, n, apply, 0)


def qkv_kernel(x_ref, te_ref, bm_ref, ang_ref, bq_ref, bk_ref, bv_ref, gq_ref, gk_ref, cgk_ref,
               ctx_hbm, wv_ref, wk_ref, wq_ref, cwk_ref, cwv_ref,
               q_out, k_out, v_out, ck_out, cv_out,
               y_ref, h_ref, ss_ref, mean_ref, cos_ref, sin_ref, vec_ref, mod_ref, qkv_ref, ctx_ref, stage_ref, ring_ref,
               ring_sem, out_sem, ctx_sem, stage_sem, send_sem, recv_sem):
    rows, width = x_ref.shape
    text = ctx_ref.shape[0]
    tn = ring_ref.shape[2]
    per = tn // 128
    nt = width // tn
    part = width // CHIPS
    n_cv = cv_out.shape[1] // tn
    me, core = my_place()
    barrier, n_signals = meet(me, core, False)
    far = (CHIPS // 2) * (1 - me // (CHIPS // 2))
    shift = far * part // tn
    ring = Ring(ring_ref, ring_sem, [(nt, w, width, tn, 1, sh, 0) for w, sh in ((wv_ref, shift), (wk_ref, 0), (wq_ref, 0), (cwk_ref, 0))]
                + [(n_cv, cwv_ref, width, tn, 1, 0, 0)])
    ring.prime()
    ctx_copy = pltpu.make_async_copy(ctx_hbm, ctx_ref, ctx_sem)
    ctx_copy.start()
    load_vectors(vec_ref, (bq_ref, bk_ref, bv_ref, gq_ref, gk_ref, cgk_ref))
    BQ, BK, BV, GQ, GK, CGK = range(6)
    mod_ref[...] = te_ref[...] + bm_ref[...]

    def vec(n, k):
        return vec_ref[n, pl.ds(k, 1), :]

    def store_y(k, val):
        y_ref[:, cols_of(k, 128)] = val.astype(BF16)

    layer_norm(lambda k: x_ref[:, cols_of(k, 128)].astype(F32), store_y,
               lambda k: 1.0 + mod_ref[SC1, pl.ds(k, 1), :], lambda k: mod_ref[SH1, pl.ds(k, 1), :],
               rows, width, ss_ref, mean_ref, False)
    pl.semaphore_wait(barrier, n_signals)

    def remote(n, dst, r):
        to = flip(me, r)
        return pltpu.make_async_remote_copy(
            src_ref=qkv_ref.at[n, :, cols_of(to, part)], dst_ref=dst.at[cols_of(me, rows)],
            send_sem=send_sem.at[n, r], recv_sem=recv_sem.at[n, r], device_id=device_at(to, core), device_id_type=MESH)

    def local(n, dst):
        return pltpu.make_async_copy(qkv_ref.at[n, :, cols_of(me, part)], dst.at[cols_of(me, rows)], out_sem.at[n])

    def q_copies():
        return [pltpu.make_async_copy(qkv_ref.at[2, :, pl.ds(d * part, part)], q_out.at[d], out_sem.at[2]) for d in range(CHIPS)]

    def v_tile(i, _):
        slot = ring.wait(0, i)
        for j in range(CHIPS // 2):
            @pl.when(i == -(-part * (j + 1) // tn))
            def _():
                remote(0, v_out, flip(me, far + j)).start()

        ct = lax.rem(i + shift, nt)
        for g, a in enumerate(groups(dot(y_ref[...], ring_ref[slot]))):
            k = ct * per + g
            qkv_ref[0, :, cols_of(k, 128)] = (a + vec(BV, k)).astype(BF16)
        ring.refill(0, i)
        return 0

    lax.fori_loop(0, nt, v_tile, 0)

    def v_rest():
        for r in range(1, CHIPS // 2):
            remote(0, v_out, r).start()
        local(0, v_out).start()
        lane = lax.broadcasted_iota(jnp.int32, (rows, HEAD), 1)
        ang = jnp.concatenate([ang_ref[...], ang_ref[...]], axis=1)
        spread = jnp.take_along_axis(ang, lane // 2, axis=1)
        cos_ref[...] = jnp.cos(spread)
        sin_ref[...] = jnp.where(lax.rem(lane, 2) == 0, -1.0, 1.0) * jnp.sin(spread)

    def k_all():
        for r in range(CHIPS - 1, 0, -1):
            remote(1, k_out, r).start()
        local(1, k_out).start()

    def q_all():
        for c in q_copies():
            c.start()
        ctx_copy.wait()

    def normed_phase(phase, n, b, gain, send_last):
        ss_ref[0:rows, :] = jnp.zeros((rows, 128), F32)

        def tile(i, _):
            slot = ring.wait(phase, i)
            pl.when(i == 0)(send_last)
            total = ss_ref[0:rows, :]
            for g, a in enumerate(groups(dot(y_ref[...], ring_ref[slot]))):
                k = i * per + g
                a = a + vec(b, k)
                h_ref[0:rows, cols_of(k, 128)] = a
                total = total + a * a
            ss_ref[0:rows, :] = total
            ring.refill(phase, i)
            return 0

        lax.fori_loop(0, nt, tile, 0)
        rms_scale(ss_ref, rows, width)
        even = lax.rem(lax.broadcasted_iota(jnp.int32, (rows, HEAD), 1), 2) == 0

        def head(j, _):
            cols = cols_of(j, HEAD)
            x = (h_ref[0:rows, cols] * ss_ref[0:rows, :]) * vec(gain, j)
            other = jnp.where(even, pltpu.roll(x, HEAD - 1, 1), pltpu.roll(x, 1, 1))
            qkv_ref[n, :, cols] = (x * cos_ref[...] + other * sin_ref[...]).astype(BF16)
            return 0

        lax.fori_loop(0, width // HEAD, head, 0)

    normed_phase(1, 1, BK, GK, v_rest)
    normed_phase(2, 2, BQ, GQ, k_all)

    def stage_copy(i, slot):
        return pltpu.make_async_copy(stage_ref.at[slot], ck_out.at[:, cols_of(i, tn)], stage_sem.at[slot])

    ss_ref[...] = jnp.zeros_like(ss_ref)

    def ck_tile(i, _):
        slot = ring.wait(3, i)
        pl.when(i == 0)(q_all)
        acc = dot(ctx_ref[...], ring_ref[slot])
        h_ref[:, cols_of(i, tn)] = acc
        add_lanes(ss_ref, text, acc, True)
        ring.refill(3, i)
        return 0

    lax.fori_loop(0, nt, ck_tile, 0)
    rms_scale(ss_ref, text, width)

    def ck_norm(i, _):
        s = lax.rem(i, 2)

        @pl.when(i >= 2)
        def _():
            stage_copy(i, s).wait()

        for j in range(per):
            k = i * per + j
            stage_ref[s, :, j * HEAD:(j + 1) * HEAD] = ((h_ref[:, cols_of(k, 128)] * ss_ref[...]) * vec(CGK, k)).astype(BF16)
        stage_copy(i, s).start()
        return 0

    lax.fori_loop(0, nt, ck_norm, 0)
    def cv_copy(i, slot):
        return pltpu.make_async_copy(stage_ref.at[slot], cv_out.at[:, cols_of(i, tn)], stage_sem.at[slot])

    def cv_tile(i, _):
        slot = ring.wait(4, i)
        s = lax.rem(nt + i, 2)
        cv_copy(i, s).wait()
        stage_ref[s] = dot(ctx_ref[...], ring_ref[slot]).astype(BF16)
        cv_copy(i, s).start()
        ring.refill(4, i)
        return 0

    lax.fori_loop(0, n_cv, cv_tile, 0)
    for i in range(2):
        stage_copy(0, i).wait()
    for c in q_copies():
        c.wait()
    for n, dst in ((0, v_out), (1, k_out)):
        local(n, dst).wait()
        for r in range(1, CHIPS):
            remote(n, dst, r).wait()


def any_spec():
    return pl.BlockSpec(memory_space=pl.ANY)


def vmem_spec():
    return pl.BlockSpec(memory_space=pltpu.VMEM)


def qkv_call(x, te, bm, ang, vectors, ctx, wv, wk, wq, cwk, cwv, cv_cols, tn):
    rows, width = x.shape
    text = ctx.shape[0]
    part = width // CHIPS
    split = jax.ShapeDtypeStruct((CHIPS, rows, part), BF16)
    gathered = jax.ShapeDtypeStruct((CHIPS * rows, part), BF16)
    flops = 2 * width * (width * (3 * rows + text) + cv_cols * text)
    return pl.pallas_call(
        qkv_kernel,
        out_shape=(split, gathered, gathered, jax.ShapeDtypeStruct((text, width), BF16), jax.ShapeDtypeStruct((text, cv_cols), BF16)),
        in_specs=[vmem_spec()] * (4 + len(vectors)) + [any_spec()] * 6,
        out_specs=[any_spec()] * 5,
        scratch_shapes=[
            pltpu.VMEM((rows, width), BF16),
            pltpu.VMEM((text, width), F32),
            pltpu.VMEM((text, 128), F32),
            pltpu.VMEM((rows, 128), F32),
            pltpu.VMEM((rows, 128), F32),
            pltpu.VMEM((rows, 128), F32),
            pltpu.VMEM((len(vectors), width // 128, 128), F32),
            pltpu.VMEM(te.shape, F32),
            pltpu.VMEM((3, rows, width), BF16),
            pltpu.VMEM((text, width), BF16),
            pltpu.VMEM((2, text, tn), BF16),
            pltpu.VMEM((3, width, tn), BF16),
            pltpu.SemaphoreType.DMA((3,)),
            pltpu.SemaphoreType.DMA((3,)),
            pltpu.SemaphoreType.DMA,
            pltpu.SemaphoreType.DMA((2,)),
            pltpu.SemaphoreType.DMA((2, CHIPS)),
            pltpu.SemaphoreType.DMA((2, CHIPS)),
        ],
        compiler_params=pltpu.CompilerParams(vmem_limit_bytes=VMEM_LIMIT, collective_id=0, has_side_effects=True),
        cost_estimate=pl.CostEstimate(flops=flops, bytes_accessed=8 * width * width, transcendentals=0),
        name='qkv',
    )(x, te, bm, ang, *vectors, ctx, wv, wk, wq, cwk, cwv)


def attend_kernel(te_ref, bm_ref, bo_ref, q_ref, k_ref, v_ref, ctx_hbm, cwv_ref, x_hbm, wo_ref, x1_out, cv_out,
                  kbuf, vbuf, qbuf, obuf, s0_ref, s1_ref, mx0_ref, mx1_ref, ctx_ref, stage_ref, ring_ref, acc_ref, wo_ring, row_ref,
                  own_sem, pair_send, pair_recv, q_send, q_recv, o_send, o_recv, ctx_sem, stage_sem, ring_sem, wo_sem):
    n_heads, keys, _ = kbuf.shape
    half = keys // 2
    rows = qbuf.shape[1]
    blocks = CHIPS * n_heads
    kb = 512 if keys % 512 == 0 else keys
    n_kb = keys // kb
    me, core = my_place()
    barrier, n_signals = meet(me, core, True)

    def own(h):
        return [pltpu.make_async_copy(src.at[:, cols_of(h, HEAD)], dst.at[h, 0:half, :], own_sem.at[n, h])
                for n, (src, dst) in enumerate(((k_ref, kbuf), (v_ref, vbuf)))]

    def pair(h):
        return [pltpu.make_async_remote_copy(
            src_ref=src.at[:, cols_of(h, HEAD)], dst_ref=dst.at[h, pl.ds(half, half), :],
            send_sem=pair_send.at[n, h], recv_sem=pair_recv.at[n, h], device_id=device_at(me, 1 - core), device_id_type=MESH)
            for n, (src, dst) in enumerate(((k_ref, kbuf), (v_ref, vbuf)))]

    def q_local():
        return pltpu.make_async_copy(q_ref.at[me], qbuf.at[0], q_recv.at[0])

    def q_remote(r):
        to = flip(me, r)
        return pltpu.make_async_remote_copy(
            src_ref=q_ref.at[to], dst_ref=qbuf.at[r], send_sem=q_send.at[r], recv_sem=q_recv.at[r],
            device_id=device_at(to, core), device_id_type=MESH)

    def o_remote(r, h):
        cols = cols_of(h, HEAD)
        return pltpu.make_async_remote_copy(
            src_ref=qbuf.at[r, :, cols], dst_ref=obuf.at[r, :, cols], send_sem=o_send.at[r, h], recv_sem=o_recv.at[r, h],
            device_id=device_at(flip(me, r), core), device_id_type=MESH)

    q_local().start()
    for h in range(n_heads):
        for c in own(h):
            c.start()
    pl.semaphore_wait(barrier, n_signals)
    for c in pair(0):
        c.start()
    for r in range(1, CHIPS):
        q_remote(r).start()
    for h in range(1, n_heads):
        for c in pair(h):
            c.start()
    tn = ring_ref.shape[2]
    nt = ring_ref.shape[1] // tn
    n_cv = cv_out.shape[1] // tn
    ring = Ring(ring_ref, ring_sem, [(n_cv, cwv_ref, ring_ref.shape[1], tn, 1, 0, nt - n_cv)])
    ring.prime()
    ctx_copy = pltpu.make_async_copy(ctx_hbm, ctx_ref, ctx_sem)
    ctx_copy.start()

    def stage_copy(i, slot):
        return pltpu.make_async_copy(stage_ref.at[slot], cv_out.at[:, cols_of(i, tn)], stage_sem.at[slot])

    def wo_copy(r, side):
        return pltpu.make_async_copy(wo_ref.at[cols_of(flip(me, r), wo_ring.shape[1]), pl.ds(side * wo_ring.shape[2], wo_ring.shape[2])],
                                     wo_ring.at[side], wo_sem.at[side])

    for side in range(2):
        wo_copy(0, side).start()

    def cv_tile(i):
        slot = ring.wait(0, i)
        s = lax.rem(i, 2)

        @pl.when(i == 0)
        def _():
            ctx_copy.wait()

        @pl.when(i >= 2)
        def _():
            stage_copy(i, s).wait()

        stage_ref[s] = dot(ctx_ref[...], ring_ref[slot]).astype(BF16)
        stage_copy(i, s).start()
        ring.refill(0, i)

    def send_output(b):
        r, h = b // n_heads, lax.rem(b, n_heads)

        @pl.when(r > 0)
        def _():
            o_remote(r, h).start()

    def step(i, now, before):
        s_now, mx_now = now
        cur = jnp.minimum(i, blocks - 1)
        r, h = cur // n_heads, lax.rem(cur, n_heads)

        @pl.when(i < n_heads)
        def _():
            for c in own(h):
                c.wait()
            for c in pair(h):
                c.wait_recv()

        @pl.when(i == 0)
        def _():
            q_local().wait()

        @pl.when((i > 0) & (i < blocks) & (h == 0))
        def _():
            q_remote(r).wait_recv()

        if before is not None:
            @pl.when(i >= 2)
            def _():
                send_output(i - 2)

            s_old, mx_old = before
            old_r, old_h = (i - 1) // n_heads, lax.rem(i - 1, n_heads)
            total = jnp.zeros((rows, 128), F32)
            acc = jnp.zeros((rows, HEAD), F32)
        q = qbuf[r, :, cols_of(h, HEAD)]
        mx = None
        for j in range(n_kb):
            s = dot_nt(q, kbuf[h, j * kb:(j + 1) * kb, :])
            s_now[:, j * kb:(j + 1) * kb] = s
            for g in range(kb // 128):
                sg = s[:, g * 128:(g + 1) * 128]
                mx = sg if mx is None else jnp.maximum(mx, sg)
            if before is not None:
                parts = []
                for g in range(kb // 128):
                    c0 = j * kb + g * 128
                    p = jnp.exp2((s_old[:, c0:c0 + 128] - mx_old[...]) * SM_C)
                    total = total + p
                    parts.append(p.astype(BF16))
                acc = acc + dot(jnp.concatenate(parts, axis=1), vbuf[old_h, j * kb:(j + 1) * kb, :])
        mx_now[...] = jnp.broadcast_to(jnp.max(mx, axis=1, keepdims=True), (rows, 128))
        if before is not None:
            qbuf[old_r, :, cols_of(old_h, HEAD)] = (acc / jnp.sum(total, axis=1, keepdims=True)).astype(BF16)

    bufs = ((s0_ref, mx0_ref), (s1_ref, mx1_ref))
    step(jnp.int32(0), bufs[0], None)

    def pair_of_steps(t, _):
        step(2 * t + 1, bufs[1], bufs[0])
        step(2 * t + 2, bufs[0], bufs[1])

        @pl.when((lax.rem(t, every) == 0) & (t < n_cv * every))
        def _():
            cv_tile(t // every)

        return 0

    every = max(1, blocks // 2 // n_cv)
    lax.fori_loop(0, blocks // 2, pair_of_steps, 0)
    send_output(jnp.int32(blocks - 1))
    for i in range(2):
        stage_copy(0, i).wait()
    width = acc_ref.shape[1]
    part = qbuf.shape[2]
    half_n = width // 2
    x_copy = pltpu.make_async_copy(x_hbm, ctx_ref.at[0:rows], ctx_sem)
    x_copy.start()
    row_ref[0] = te_ref[G1] + bm_ref[G1]
    row_ref[1] = bo_ref[...].astype(F32)

    def project(r, lhs, side, finish):
        wo_copy(r, side).wait()
        for n in range(half_n // tn):
            cols = pl.ds(side * half_n + n * tn, tn)
            finish(cols, side * half_n + n * tn, dot(lhs[...], wo_ring[side, :, n * tn:(n + 1) * tn]))

    def first(cols, c0, prod):
        acc_ref[:, cols] = prod

    def middle(cols, c0, prod):
        acc_ref[:, cols] = acc_ref[:, cols] + prod

    def last(cols, c0, prod):
        for g, p in enumerate(groups(prod)):
            k = c0 // 128 + g
            gc = slice(c0 + g * 128, c0 + (g + 1) * 128)
            acc_ref[:, gc] = ctx_ref[0:rows, gc].astype(F32) + row_ref[0, k:k + 1, :] * (acc_ref[:, gc] + p + row_ref[1, k:k + 1, :])

    def arrived(r):
        for h in range(n_heads):
            o_remote(r, h).wait_recv()

    def x1_copy(side):
        cols = pl.ds(side * half_n, half_n)
        return pltpu.make_async_copy(acc_ref.at[:, cols], x1_out.at[:, cols], stage_sem.at[side])

    for side in range(2):
        project(0, qbuf.at[0], side, first)
        wo_copy(1, side).start()

    def chunk(r, _):
        arrived(r)
        for side in range(2):
            project(r, obuf.at[r], side, middle)
            wo_copy(r + 1, side).start()
        return 0

    lax.fori_loop(1, CHIPS - 1, chunk, 0)
    x_copy.wait()
    arrived(CHIPS - 1)
    project(CHIPS - 1, obuf.at[CHIPS - 1], 0, last)
    project(CHIPS - 1, obuf.at[CHIPS - 1], 1, last)
    x1_copy(0).start()
    for h in range(n_heads):
        for c in pair(h):
            c.wait_send()

    def drain(r, _):
        q_remote(r).wait_send()
        for h in range(n_heads):
            o_remote(r, h).wait_send()
        return 0

    lax.fori_loop(1, CHIPS, drain, 0)
    x1_copy(1).start()
    for side in range(2):
        x1_copy(side).wait()


def attend_call(te, bm, bo, q, k, v, ctx, cwv, x, wo, cv_cols, tn):
    _, rows, part = q.shape
    half = k.shape[0]
    n_heads = part // HEAD
    text, width = ctx.shape
    flops = 8 * half * half * part + 2 * width * (text * cv_cols + rows * width)
    return pl.pallas_call(
        attend_kernel,
        out_shape=(jax.ShapeDtypeStruct((rows, width), F32), jax.ShapeDtypeStruct((text, cv_cols), BF16)),
        in_specs=[vmem_spec()] * 3 + [any_spec()] * 7,
        out_specs=[any_spec()] * 2,
        scratch_shapes=[
            pltpu.VMEM((n_heads, 2 * half, HEAD), BF16),
            pltpu.VMEM((n_heads, 2 * half, HEAD), BF16),
            pltpu.VMEM((CHIPS, rows, part), BF16),
            pltpu.VMEM((CHIPS, rows, part), BF16),
            pltpu.VMEM((rows, 2 * half), F32),
            pltpu.VMEM((rows, 2 * half), F32),
            pltpu.VMEM((rows, 128), F32),
            pltpu.VMEM((rows, 128), F32),
            pltpu.VMEM((text, width), BF16),
            pltpu.VMEM((2, text, tn), BF16),
            pltpu.VMEM((2, width, tn), BF16),
            pltpu.VMEM((rows, width), F32),
            pltpu.VMEM((2, part, width // 2), BF16),
            pltpu.VMEM((2, width // 128, 128), F32),
            pltpu.SemaphoreType.DMA((2, n_heads)),
            pltpu.SemaphoreType.DMA((2, n_heads)),
            pltpu.SemaphoreType.DMA((2, n_heads)),
            pltpu.SemaphoreType.DMA((CHIPS,)),
            pltpu.SemaphoreType.DMA((CHIPS,)),
            pltpu.SemaphoreType.DMA((CHIPS, n_heads)),
            pltpu.SemaphoreType.DMA((CHIPS, n_heads)),
            pltpu.SemaphoreType.DMA,
            pltpu.SemaphoreType.DMA((2,)),
            pltpu.SemaphoreType.DMA((2,)),
            pltpu.SemaphoreType.DMA((2,)),
        ],
        compiler_params=pltpu.CompilerParams(vmem_limit_bytes=VMEM_LIMIT, collective_id=1, has_side_effects=True),
        cost_estimate=pl.CostEstimate(flops=flops, bytes_accessed=8 * half * part + 4 * width * width, transcendentals=2 * half * half * n_heads),
        name='attend',
    )(te, bm, bo, q, k, v, ctx, cwv, x, wo)


class Slabs:
    def __init__(self, slots, sems, phases):
        self.slots, self.sems, self.phases = slots, sems, phases
        self.depth, self.rows = slots.shape[0], slots.shape[1]
        self.base = [sum(p[0] for p in phases[:i]) for i in range(len(phases) + 1)]

    def copies(self, phase, i):
        n, w_ref, n_k, n_cols = self.phases[phase]
        slot = lax.rem(self.base[phase] + i, self.depth)
        cols = cols_of(i // n_k, n_cols)
        quarter = self.rows // 4
        return [pltpu.make_async_copy(w_ref.at[cols_of(lax.rem(i, n_k) * 4 + c, quarter), cols],
                                      self.slots.at[slot, pl.ds(c * quarter, quarter), pl.ds(0, n_cols)], self.sems.at[slot]) for c in range(4)]

    def start(self, phase, i):
        for c in self.copies(phase, i):
            c.start()

    def prime(self):
        for i in range(self.depth):
            self.start(0, i)

    def add_product(self, phase, i, lhs, k, acc_ref):
        n, _, _, n_cols = self.phases[phase]
        for c in self.copies(phase, i):
            c.wait()
        slot = lax.rem(self.base[phase] + i, self.depth)
        per = self.rows // 128
        left = jnp.concatenate([lhs[k * per + g] for g in range(per)], axis=1)
        c0 = 0
        while c0 < n_cols:
            cols = slice(c0, min(c0 + 512, n_cols))
            acc_ref[:, cols] = acc_ref[:, cols] + dot(left, self.slots[slot, :, cols])
            c0 += 512
        ahead = i + self.depth

        @pl.when(ahead < n)
        def _():
            self.start(phase, ahead)

        if phase + 1 < len(self.phases):
            @pl.when(ahead >= n)
            def _():
                self.start(phase + 1, ahead - n)


def tail_kernel(te_ref, bm_ref, nw_ref, nb_ref, cgq_ref, x1_ref, ck_ref, cva_ref, cvb_ref, cwq_ref, cwo_ref, w1_ref, w2_ref,
                out_ref, a_ref, b_ref, xf_ref, h_ref, u_ref, ss_ref, mean_ref, vec_ref, mod_ref, kbuf, vbuf,
                s0_ref, s1_ref, s2_ref, s3_ref, stage_ref, slab_ref, slab_sem, in_sem, kv_sem, stage_sem):
    rows, width = xf_ref.shape
    ff = u_ref.shape[0] * 128
    text = kbuf.shape[1]
    tn = slab_ref.shape[1]
    per = tn // 128
    nt = width // tn
    n_k2 = ff // tn
    blocks = -(-ff // width)
    bc = ff // blocks
    slabs = Slabs(slab_ref, slab_sem, [
        (nt, cwq_ref, nt, width), (nt, cwo_ref, nt, width), (nt * blocks, w1_ref, nt, bc), (n_k2, w2_ref, n_k2, width)])
    x1_copy = pltpu.make_async_copy(x1_ref, xf_ref, in_sem)
    x1_copy.start()
    slabs.prime()
    load_vectors(vec_ref, (nw_ref, nb_ref, cgq_ref))
    NW, NB, CGQ = range(3)
    mod_ref[...] = te_ref[...] + bm_ref[...]

    def vec(n, k):
        return vec_ref[n, pl.ds(k, 1), :]

    def mod(n, k):
        return mod_ref[n, pl.ds(k, 1), :]

    def clear(ref):
        def body(j, _):
            ref[:, cols_of(j, tn)] = jnp.zeros((rows, tn), F32)
            return 0

        lax.fori_loop(0, nt, body, 0)

    clear(h_ref)
    x1_copy.wait()

    def norm_to(dst, mul, add):
        def store(k, val):
            dst[k] = val.astype(BF16)

        layer_norm(lambda k: xf_ref[:, cols_of(k, 128)], store, mul, add, rows, width, ss_ref, mean_ref, False)

    norm_to(b_ref, lambda k: vec(NW, k), lambda k: vec(NB, k))

    def cq_slab(i, _):
        slabs.add_product(0, i, b_ref, i, h_ref)
        return 0

    lax.fori_loop(0, nt, cq_slab, 0)
    gw = kbuf.shape[2]
    n_groups = width // gw
    heads = gw // HEAD
    n_cva = cva_ref.shape[1] // gw

    def kv_loads(g, slot):
        return (pltpu.make_async_copy(ck_ref.at[:, cols_of(g, gw)], kbuf.at[slot], kv_sem.at[0, slot]),
                pltpu.make_async_copy(cva_ref.at[:, cols_of(jnp.minimum(g, n_cva - 1), gw)], vbuf.at[slot], kv_sem.at[1, slot]),
                pltpu.make_async_copy(cvb_ref.at[:, cols_of(jnp.maximum(g - n_cva, 0), gw)], vbuf.at[slot], kv_sem.at[1, slot]))

    def kv_start(g, slot):
        k_copy, va_copy, vb_copy = kv_loads(g, slot)
        k_copy.start()

        @pl.when(g < n_cva)
        def _():
            va_copy.start()

        @pl.when(g >= n_cva)
        def _():
            vb_copy.start()

    kv_start(jnp.int32(0), jnp.int32(0))
    ss_ref[...] = jnp.zeros_like(ss_ref)

    def cq_squares(i, _):
        add_lanes(ss_ref, rows, h_ref[:, cols_of(i, tn)], True)
        return 0

    lax.fori_loop(0, nt, cq_squares, 0)
    rms_scale(ss_ref, rows, width)

    def cq_head(i, _):
        for g in range(per):
            k = i * per + g
            a_ref[k] = ((h_ref[:, cols_of(k, 128)] * ss_ref[...]) * vec(CGQ, k)).astype(BF16)
        return 0

    lax.fori_loop(0, nt, cq_head, 0)
    s_refs = (s0_ref, s1_ref, s2_ref, s3_ref)

    def cross_group(g, _):
        slot = lax.rem(g, 2)
        k_copy, v_copy, _ = kv_loads(g, slot)
        k_copy.wait()
        v_copy.wait()

        @pl.when(g + 1 < n_groups)
        def _():
            kv_start(g + 1, 1 - slot)

        tops = []

        def score(j):
            s = dot_nt(a_ref[g * heads + j], kbuf[slot, :, j * HEAD:(j + 1) * HEAD])
            s_refs[j % 4][...] = s
            parts = groups(s)
            mx = parts[0]
            for p in parts[1:]:
                mx = jnp.maximum(mx, p)
            tops.append(jnp.broadcast_to(jnp.max(mx, axis=1, keepdims=True), (rows, 128)))

        def weigh(j):
            total = jnp.zeros((rows, 128), F32)
            parts = []
            for c in range(text // 128):
                p = jnp.exp2((s_refs[j % 4][:, c * 128:(c + 1) * 128] - tops[j]) * SM_C)
                total = total + p
                parts.append(p.astype(BF16))
            acc = dot(jnp.concatenate(parts, axis=1), vbuf[slot, :, j * HEAD:(j + 1) * HEAD])
            b_ref[g * heads + j] = (acc / jnp.sum(total, axis=1, keepdims=True)).astype(BF16)

        score(0)
        for j in range(1, heads):
            score(j)
            weigh(j - 1)
        weigh(heads - 1)
        return 0

    lax.fori_loop(0, n_groups, cross_group, 0)

    def co_slab(i, _):
        slabs.add_product(1, i, b_ref, i, xf_ref)
        return 0

    lax.fori_loop(0, nt, co_slab, 0)
    norm_to(a_ref, lambda k: 1.0 + mod(SC2, k), lambda k: mod(SH2, k))

    def f1_block(c, _):
        clear(h_ref)

        def f1_slab(k, _):
            slabs.add_product(2, c * nt + k, a_ref, k, h_ref)
            return 0

        lax.fori_loop(0, nt, f1_slab, 0)

        def gelu(j, _):
            u_ref[c * (bc // 128) + j] = jax.nn.gelu(h_ref[:, cols_of(j, 128)], approximate=True).astype(BF16)
            return 0

        lax.fori_loop(0, bc // 128, gelu, 0)
        return 0

    lax.fori_loop(0, blocks, f1_block, 0)
    clear(h_ref)

    def f2_slab(k, _):
        slabs.add_product(3, k, u_ref, k, h_ref)
        return 0

    lax.fori_loop(0, n_k2, f2_slab, 0)

    def stage_copy(i, slot):
        return pltpu.make_async_copy(stage_ref.at[slot], out_ref.at[:, cols_of(i, tn)], stage_sem.at[slot])

    def finish(i, _):
        s = lax.rem(i, 2)

        @pl.when(i >= 2)
        def _():
            stage_copy(i, s).wait()

        for g in range(per):
            k = i * per + g
            stage_ref[s, :, g * 128:(g + 1) * 128] = (xf_ref[:, cols_of(k, 128)] + mod(G2, k) * h_ref[:, cols_of(k, 128)]).astype(BF16)
        stage_copy(i, s).start()
        return 0

    lax.fori_loop(0, nt, finish, 0)
    for i in range(2):
        stage_copy(0, i).wait()


def tail_call(te, bm, vectors, x1, ck, cva, cvb, cwq, cwo, w1, w2, tn):
    rows, width = x1.shape
    text = ck.shape[0]
    ff = w1.shape[1]
    depth = 4
    flops = 2 * rows * width * (2 * width + 2 * ff) + 4 * rows * text * width
    return pl.pallas_call(
        tail_kernel,
        out_shape=jax.ShapeDtypeStruct((rows, width), BF16),
        in_specs=[vmem_spec()] * (2 + len(vectors)) + [any_spec()] * 8,
        out_specs=any_spec(),
        scratch_shapes=[
            pltpu.VMEM((width // 128, rows, 128), BF16),
            pltpu.VMEM((width // 128, rows, 128), BF16),
            pltpu.VMEM((rows, width), F32),
            pltpu.VMEM((rows, width), F32),
            pltpu.VMEM((ff // 128, rows, 128), BF16),
            pltpu.VMEM((rows, 128), F32),
            pltpu.VMEM((rows, 128), F32),
            pltpu.VMEM((len(vectors), width // 128, 128), F32),
            pltpu.VMEM(te.shape, F32),
            pltpu.VMEM((2, text, 8 * HEAD), BF16),
            pltpu.VMEM((2, text, 8 * HEAD), BF16),
            pltpu.VMEM((rows, text), F32),
            pltpu.VMEM((rows, text), F32),
            pltpu.VMEM((rows, text), F32),
            pltpu.VMEM((rows, text), F32),
            pltpu.VMEM((2, rows, tn), BF16),
            pltpu.VMEM((depth, tn, width), BF16),
            pltpu.SemaphoreType.DMA((depth,)),
            pltpu.SemaphoreType.DMA,
            pltpu.SemaphoreType.DMA((2, 2)),
            pltpu.SemaphoreType.DMA((2,)),
        ],
        compiler_params=pltpu.CompilerParams(vmem_limit_bytes=VMEM_LIMIT),
        cost_estimate=pl.CostEstimate(flops=flops, bytes_accessed=2 * width * (2 * width + 2 * ff), transcendentals=rows * ff),
        name='tail',
    )(te, bm, *vectors, x1, ck, cva, cvb, cwq, cwo, w1, w2)


def solution(mesh):
    tok_spec = P('dp', ('sp', 'uly'), None)
    batch_spec = P('dp', None, None)

    def local_block(tokens, rope_ang, t_emb, block_mod, context, attn_wq, attn_bq, attn_wk, attn_bk, attn_wv, attn_bv, attn_gq, attn_gk, attn_wo, attn_bo, norm3_w, norm3_b, cross_wq, cross_wk, cross_wv, cross_gq, cross_gk, cross_wo, ffn_w1, ffn_w2):
        x, ctx = tokens[0], context[0]
        te, bm = (m.reshape(6, -1, 128) for m in (t_emb, block_mod))
        tn = min(512, x.shape[1] // CHIPS)

        def lanes(*vectors):
            return tuple(v.reshape(-1, 128) for v in vectors)

        cv_a = max(1024, x.shape[1] * 2 // 5 // 1024 * 1024)
        cv_b = x.shape[1] - cv_a
        q, k, v, ck, cva = qkv_call(x, te, bm, rope_ang, lanes(attn_bq, attn_bk, attn_bv, attn_gq, attn_gk, cross_gk), ctx,
                                    attn_wv, attn_wk, attn_wq, cross_wk, cross_wv, cv_a, tn)
        x1, cvb = attend_call(te, bm, *lanes(attn_bo), q, k, v, ctx, cross_wv, x, attn_wo, cv_b, tn)
        out = tail_call(te, bm, lanes(norm3_w, norm3_b, cross_gq), x1, ck, cva, cvb, cross_wq, cross_wo, ffn_w1, ffn_w2, tn)
        return out[None]

    in_specs = (tok_spec, P(('sp', 'uly'), None), batch_spec, P(), batch_spec) + (P(),) * 20
    return jax.shard_map(local_block, mesh=mesh, in_specs=in_specs, out_specs=tok_spec, check_vma=False)
```

```python
import functools

import jax
import jax.numpy as jnp
from jax import lax
from jax.experimental import pallas as pl
from jax.experimental.pallas import tpu as pltpu
from jax.sharding import PartitionSpec as P

EPS = 1e-6
HEAD = 128
LOG2E = 1.4426950408889634
GELU_A = 0.7978845608028654
SM_C = (HEAD ** -0.5) * LOG2E
MESH = pl.DeviceIdType.MESH
CHIPS = 8
VMEM_LIMIT = 64 * 1000 * 1024
F32 = jnp.float32
BF16 = jnp.bfloat16

SH1, SC1, G1, SH2, SC2, G2 = range(6)


def dot(a, b):
    return jnp.dot(a, b, preferred_element_type=F32)


def dot_nt(a, b):
    return lax.dot_general(a, b, (((1,), (1,)), ((), ())), preferred_element_type=F32)


def gelu_tanh(x):
    half = 0.5 * x
    return half + half * jnp.tanh(x * (GELU_A + (GELU_A * 0.044715) * (x * x)))


def my_place():
    uly = lax.axis_index('uly')
    chip = lax.axis_index('sp') * 2 + uly // 2
    return chip, lax.rem(uly, 2)


def device_at(chip, core):
    return {'sp': chip // 2, 'uly': lax.rem(chip, 2) * 2 + core}


def flip(chip, r):
    out = 0
    for bit in (1, 2, 4):
        out = out + lax.rem(chip // bit + r // bit, 2) * bit
    return out


def meet(me, core, sibling):
    barrier = pltpu.get_barrier_semaphore()
    for r in range(1, CHIPS):
        pl.semaphore_signal(barrier, inc=1, device_id=device_at(flip(me, r), core), device_id_type=MESH)
    if sibling:
        pl.semaphore_signal(barrier, inc=1, device_id=device_at(me, 1 - core), device_id_type=MESH)
    return barrier, CHIPS - 1 + int(sibling)


class Ring:
    def __init__(self, slots, sems, phases):
        self.slots, self.sems, self.phases = slots, sems, phases
        self.depth = slots.shape[0]
        self.base = [sum(p[0] for p in phases[:i]) for i in range(len(phases) + 1)]

    def slot(self, phase, tile):
        return lax.rem(self.base[phase] + tile, self.depth)

    def copies(self, phase, tile):
        n, w_ref, k_rows, n_cols, k_parts, shift, col0 = self.phases[phase]
        slot = self.slot(phase, tile)
        cols = cols_of(col0 + lax.rem(tile // k_parts + shift, n // k_parts), n_cols)
        row0 = lax.rem(tile, k_parts) * k_rows
        quarter = k_rows // 4
        out = []
        for c in range(4):
            rows = pl.ds(pl.multiple_of(row0 + c * quarter, quarter), quarter)
            out.append(pltpu.make_async_copy(w_ref.at[rows, cols], self.slots.at[slot, pl.ds(c * quarter, quarter)], self.sems.at[slot]))
        return out

    def start(self, phase, tile):
        for c in self.copies(phase, tile):
            c.start()

    def prime(self):
        for i in range(self.depth):
            if i < self.phases[0][0]:
                self.start(0, i)
            else:
                self.start(1, i - self.phases[0][0])

    def wait(self, phase, tile):
        for c in self.copies(phase, tile):
            c.wait()
        return self.slot(phase, tile)

    def refill(self, phase, tile):
        n = self.phases[phase][0]
        ahead = tile + self.depth

        @pl.when(ahead < n)
        def _():
            self.start(phase, ahead)

        if phase + 1 < len(self.phases):
            @pl.when(ahead >= n)
            def _():
                self.start(phase + 1, ahead - n)


def cols_of(i, width):
    return pl.ds(pl.multiple_of(i * width, width), width)


def groups(acc):
    return [acc[:, g * 128:(g + 1) * 128] for g in range(acc.shape[1] // 128)]


def add_lanes(ref, rows, acc, squares):
    total = ref[0:rows, :]
    for part in groups(acc):
        total = total + (part * part if squares else part)
    ref[0:rows, :] = total


def lane_mean(ref, rows, width):
    return jnp.broadcast_to(jnp.sum(ref[0:rows, :], axis=1, keepdims=True) * (1.0 / width), (rows, 128))


def rms_scale(ss_ref, rows, width):
    ss_ref[0:rows, :] = lax.rsqrt(lane_mean(ss_ref, rows, width) + EPS)


def load_vectors(vec_ref, refs):
    for n, ref in enumerate(refs):
        vec_ref[n] = ref[...].astype(F32)


def layer_norm(load, store, mul, add, rows, width, sum_ref, mean_ref, have_sum):
    step = 4 if width % 512 == 0 else 1
    n = width // 128 // step

    def sums(j, _):
        total = sum_ref[0:rows, :]
        for g in range(step):
            total = total + load(j * step + g)
        sum_ref[0:rows, :] = total
        return 0

    if not have_sum:
        sum_ref[0:rows, :] = jnp.zeros((rows, 128), F32)
        lax.fori_loop(0, n, sums, 0)
    mean_ref[...] = lane_mean(sum_ref, rows, width)
    sum_ref[0:rows, :] = jnp.zeros((rows, 128), F32)

    def squares(j, _):
        total = sum_ref[0:rows, :]
        for g in range(step):
            d = load(j * step + g) - mean_ref[...]
            total = total + d * d
        sum_ref[0:rows, :] = total
        return 0

    lax.fori_loop(0, n, squares, 0)
    rms_scale(sum_ref, rows, width)

    def apply(j, _):
        for g in range(step):
            k = j * step + g
            store(k, ((load(k) - mean_ref[...]) * sum_ref[0:rows, :]) * mul(k) + add(k))
        return 0

    lax.fori_loop(0, n, apply, 0)


def qkv_kernel(x_ref, te_ref, bm_ref, ang_ref, bq_ref, bk_ref, bv_ref, gq_ref, gk_ref, cgk_ref,
               ctx_hbm, wv_ref, wk_ref, wq_ref, cwk_ref, cwv_ref,
               q_out, k_out, v_out, ck_out, cv_out,
               y_ref, h_ref, ss_ref, mean_ref, cos_ref, sin_ref, vec_ref, mod_ref, qkv_ref, ctx_ref, stage_ref, ring_ref,
               ring_sem, out_sem, ctx_sem, stage_sem, send_sem, recv_sem):
    rows, width = x_ref.shape
    text = ctx_ref.shape[0]
    tn = ring_ref.shape[2]
    per = tn // 128
    nt = width // tn
    part = width // CHIPS
    n_cv = cv_out.shape[1] // tn
    me, core = my_place()
    barrier, n_signals = meet(me, core, False)
    far = (CHIPS // 2) * (1 - me // (CHIPS // 2))
    shift = far * part // tn
    ring = Ring(ring_ref, ring_sem, [(nt, w, width, tn, 1, sh, 0) for w, sh in ((wv_ref, shift), (wk_ref, 0), (wq_ref, 0), (cwk_ref, 0))]
                + [(n_cv, cwv_ref, width, tn, 1, 0, 0)])
    ring.prime()
    ctx_copy = pltpu.make_async_copy(ctx_hbm, ctx_ref, ctx_sem)
    ctx_copy.start()
    load_vectors(vec_ref, (bq_ref, bk_ref, bv_ref, gq_ref, gk_ref, cgk_ref))
    BQ, BK, BV, GQ, GK, CGK = range(6)
    mod_ref[...] = te_ref[...] + bm_ref[...]

    def vec(n, k):
        return vec_ref[n, pl.ds(k, 1), :]

    def store_y(k, val):
        y_ref[:, cols_of(k, 128)] = val.astype(BF16)

    layer_norm(lambda k: x_ref[:, cols_of(k, 128)].astype(F32), store_y,
               lambda k: 1.0 + mod_ref[SC1, pl.ds(k, 1), :], lambda k: mod_ref[SH1, pl.ds(k, 1), :],
               rows, width, ss_ref, mean_ref, False)
    pl.semaphore_wait(barrier, n_signals)

    def remote(n, dst, r):
        to = flip(me, r)
        return pltpu.make_async_remote_copy(
            src_ref=qkv_ref.at[n, :, cols_of(to, part)], dst_ref=dst.at[cols_of(me, rows)],
            send_sem=send_sem.at[n, r], recv_sem=recv_sem.at[n, r], device_id=device_at(to, core), device_id_type=MESH)

    def local(n, dst):
        return pltpu.make_async_copy(qkv_ref.at[n, :, cols_of(me, part)], dst.at[cols_of(me, rows)], out_sem.at[n])

    def q_copies():
        return [pltpu.make_async_copy(qkv_ref.at[2, :, pl.ds(d * part, part)], q_out.at[d], out_sem.at[2]) for d in range(CHIPS)]

    def far_pieces(t):
        out = []
        for j in range(CHIPS // 2):
            lo, hi = max(t * tn, j * part), min((t + 1) * tn, (j + 1) * part)
            if lo < hi:
                src = pl.ds(pl.multiple_of(far * part + lo, 128), hi - lo)
                r = flip(me, far + j)
                out.append(pltpu.make_async_remote_copy(
                    src_ref=qkv_ref.at[0, :, src], dst_ref=v_out.at[cols_of(me, rows), pl.ds(lo - j * part, hi - lo)],
                    send_sem=send_sem.at[0, r], recv_sem=recv_sem.at[0, r], device_id=device_at(far + j, core), device_id_type=MESH))
        return out

    def v_tile(i, _):
        slot = ring.wait(0, i)
        for t in range(nt // 2):
            @pl.when(i == t + 1)
            def _():
                for c in far_pieces(t):
                    c.start()

        ct = lax.rem(i + shift, nt)
        for g, a in enumerate(groups(dot(y_ref[...], ring_ref[slot]))):
            k = ct * per + g
            qkv_ref[0, :, cols_of(k, 128)] = (a + vec(BV, k)).astype(BF16)
        ring.refill(0, i)
        return 0

    lax.fori_loop(0, nt, v_tile, 0)

    def v_rest():
        for r in range(1, CHIPS // 2):
            remote(0, v_out, r).start()
        local(0, v_out).start()
        pick = (lax.broadcasted_iota(jnp.int32, (HEAD // 2, HEAD), 1) // 2 == lax.broadcasted_iota(jnp.int32, (HEAD // 2, HEAD), 0)).astype(F32)
        sign = 2.0 * lax.rem(lax.broadcasted_iota(jnp.int32, (HEAD // 2, HEAD), 1), 2).astype(F32) - 1.0

        def spread(table, picker):
            return lax.dot_general(table, picker, (((0,), (0,)), ((), ())), precision=lax.Precision.HIGHEST, preferred_element_type=F32)

        cos_ref[...] = spread(jnp.cos(ang_ref[...]), pick)
        sin_ref[...] = spread(jnp.sin(ang_ref[...]), pick * sign)

    def k_all():
        for r in range(CHIPS - 1, 0, -1):
            remote(1, k_out, r).start()
        local(1, k_out).start()

    def q_all():
        for c in q_copies():
            c.start()
        ctx_copy.wait()

    def normed_phase(phase, n, b, gain, send_last):
        ss_ref[0:rows, :] = jnp.zeros((rows, 128), F32)

        def tile(i, _):
            slot = ring.wait(phase, i)
            pl.when(i == 0)(send_last)
            total = ss_ref[0:rows, :]
            for g, a in enumerate(groups(dot(y_ref[...], ring_ref[slot]))):
                k = i * per + g
                a = a + vec(b, k)
                h_ref[0:rows, cols_of(k, 128)] = a
                total = total + a * a
            ss_ref[0:rows, :] = total
            ring.refill(phase, i)
            return 0

        lax.fori_loop(0, nt, tile, 0)
        rms_scale(ss_ref, rows, width)
        even = lax.rem(lax.broadcasted_iota(jnp.int32, (rows, HEAD), 1), 2) == 0

        def head(j, _):
            cols = cols_of(j, HEAD)
            x = (h_ref[0:rows, cols] * ss_ref[0:rows, :]) * vec(gain, j)
            other = jnp.where(even, pltpu.roll(x, HEAD - 1, 1), pltpu.roll(x, 1, 1))
            qkv_ref[n, :, cols] = (x * cos_ref[...] + other * sin_ref[...]).astype(BF16)
            return 0

        lax.fori_loop(0, width // HEAD, head, 0)

    normed_phase(1, 1, BK, GK, v_rest)
    normed_phase(2, 2, BQ, GQ, k_all)

    def stage_copy(i, slot):
        return pltpu.make_async_copy(stage_ref.at[slot], ck_out.at[:, cols_of(i, tn)], stage_sem.at[slot])

    ss_ref[...] = jnp.zeros_like(ss_ref)

    def ck_tile(i, _):
        slot = ring.wait(3, i)
        pl.when(i == 0)(q_all)
        acc = dot(ctx_ref[...], ring_ref[slot])
        h_ref[:, cols_of(i, tn)] = acc
        add_lanes(ss_ref, text, acc, True)
        ring.refill(3, i)
        return 0

    lax.fori_loop(0, nt, ck_tile, 0)
    rms_scale(ss_ref, text, width)

    def ck_norm(i, _):
        s = lax.rem(i, 2)

        @pl.when(i >= 2)
        def _():
            stage_copy(i, s).wait()

        for j in range(per):
            k = i * per + j
            stage_ref[s, :, j * HEAD:(j + 1) * HEAD] = ((h_ref[:, cols_of(k, 128)] * ss_ref[...]) * vec(CGK, k)).astype(BF16)
        stage_copy(i, s).start()
        return 0

    lax.fori_loop(0, nt, ck_norm, 0)
    def cv_copy(i, slot):
        return pltpu.make_async_copy(stage_ref.at[slot], cv_out.at[:, cols_of(i, tn)], stage_sem.at[slot])

    def cv_tile(i, _):
        slot = ring.wait(4, i)
        s = lax.rem(nt + i, 2)
        cv_copy(i, s).wait()
        stage_ref[s] = dot(ctx_ref[...], ring_ref[slot]).astype(BF16)
        cv_copy(i, s).start()
        ring.refill(4, i)
        return 0

    lax.fori_loop(0, n_cv, cv_tile, 0)
    for i in range(2):
        stage_copy(0, i).wait()
    for c in q_copies():
        c.wait()
    for n, dst in ((0, v_out), (1, k_out)):
        local(n, dst).wait()
        for r in range(1, CHIPS):
            remote(n, dst, r).wait()


def any_spec():
    return pl.BlockSpec(memory_space=pl.ANY)


def vmem_spec():
    return pl.BlockSpec(memory_space=pltpu.VMEM)


def qkv_call(x, te, bm, ang, vectors, ctx, wv, wk, wq, cwk, cwv, cv_cols, tn):
    rows, width = x.shape
    text = ctx.shape[0]
    part = width // CHIPS
    split = jax.ShapeDtypeStruct((CHIPS, rows, part), BF16)
    gathered = jax.ShapeDtypeStruct((CHIPS * rows, part), BF16)
    flops = 2 * width * (width * (3 * rows + text) + cv_cols * text)
    return pl.pallas_call(
        qkv_kernel,
        out_shape=(split, gathered, gathered, jax.ShapeDtypeStruct((text, width), BF16), jax.ShapeDtypeStruct((text, cv_cols), BF16)),
        in_specs=[vmem_spec()] * (4 + len(vectors)) + [any_spec()] * 6,
        out_specs=[any_spec()] * 5,
        scratch_shapes=[
            pltpu.VMEM((rows, width), BF16),
            pltpu.VMEM((text, width), F32),
            pltpu.VMEM((text, 128), F32),
            pltpu.VMEM((rows, 128), F32),
            pltpu.VMEM((rows, 128), F32),
            pltpu.VMEM((rows, 128), F32),
            pltpu.VMEM((len(vectors), width // 128, 128), F32),
            pltpu.VMEM(te.shape, F32),
            pltpu.VMEM((3, rows, width), BF16),
            pltpu.VMEM((text, width), BF16),
            pltpu.VMEM((2, text, tn), BF16),
            pltpu.VMEM((3, width, tn), BF16),
            pltpu.SemaphoreType.DMA((3,)),
            pltpu.SemaphoreType.DMA((3,)),
            pltpu.SemaphoreType.DMA,
            pltpu.SemaphoreType.DMA((2,)),
            pltpu.SemaphoreType.DMA((2, CHIPS)),
            pltpu.SemaphoreType.DMA((2, CHIPS)),
        ],
        compiler_params=pltpu.CompilerParams(vmem_limit_bytes=VMEM_LIMIT, collective_id=0, has_side_effects=True),
        cost_estimate=pl.CostEstimate(flops=flops, bytes_accessed=8 * width * width, transcendentals=0),
        name='qkv',
    )(x, te, bm, ang, *vectors, ctx, wv, wk, wq, cwk, cwv)


def attend_kernel(te_ref, bm_ref, bo_ref, q_ref, k_ref, v_ref, ctx_hbm, cwv_ref, x_hbm, wo_ref, x1_out, sum_out, cv_out,
                  kbuf, vbuf, qbuf, obuf, s0_ref, s1_ref, mx0_ref, mx1_ref, ctx_ref, stage_ref, ring_ref, acc_ref, wo_ring, row_ref,
                  own_sem, pair_send, pair_recv, q_send, q_recv, o_send, o_recv, ctx_sem, stage_sem, ring_sem, wo_sem, x_sem):
    n_heads, keys, _ = kbuf.shape
    half = keys // 2
    rows = qbuf.shape[1]
    blocks = CHIPS * n_heads
    kb = 512 if keys % 512 == 0 else keys
    n_kb = keys // kb
    me, core = my_place()
    barrier, n_signals = meet(me, core, True)

    def own(h):
        return [pltpu.make_async_copy(src.at[:, cols_of(h, HEAD)], dst.at[h, 0:half, :], own_sem.at[n, h])
                for n, (src, dst) in enumerate(((k_ref, kbuf), (v_ref, vbuf)))]

    def pair(h):
        return [pltpu.make_async_remote_copy(
            src_ref=src.at[:, cols_of(h, HEAD)], dst_ref=dst.at[h, pl.ds(half, half), :],
            send_sem=pair_send.at[n, h], recv_sem=pair_recv.at[n, h], device_id=device_at(me, 1 - core), device_id_type=MESH)
            for n, (src, dst) in enumerate(((k_ref, kbuf), (v_ref, vbuf)))]

    def q_local():
        return pltpu.make_async_copy(q_ref.at[me], qbuf.at[0], q_recv.at[0])

    def q_remote(r):
        to = flip(me, r)
        return pltpu.make_async_remote_copy(
            src_ref=q_ref.at[to], dst_ref=qbuf.at[r], send_sem=q_send.at[r], recv_sem=q_recv.at[r],
            device_id=device_at(to, core), device_id_type=MESH)

    def o_remote(r, h):
        cols = cols_of(h, HEAD)
        return pltpu.make_async_remote_copy(
            src_ref=qbuf.at[r, :, cols], dst_ref=obuf.at[r, :, cols], send_sem=o_send.at[r, h], recv_sem=o_recv.at[r, h],
            device_id=device_at(flip(me, r), core), device_id_type=MESH)

    q_local().start()
    for h in range(n_heads):
        for c in own(h):
            c.start()
    pl.semaphore_wait(barrier, n_signals)
    for c in pair(0):
        c.start()
    for r in range(1, CHIPS):
        q_remote(r).start()
    for h in range(1, n_heads):
        for c in pair(h):
            c.start()
    tn = ring_ref.shape[2]
    nt = ring_ref.shape[1] // tn
    n_cv = cv_out.shape[1] // tn
    ring = Ring(ring_ref, ring_sem, [(n_cv, cwv_ref, ring_ref.shape[1], tn, 1, 0, nt - n_cv)])
    ring.prime()
    ctx_copy = pltpu.make_async_copy(ctx_hbm, ctx_ref, ctx_sem)
    ctx_copy.start()

    def stage_copy(i, slot):
        return pltpu.make_async_copy(stage_ref.at[slot], cv_out.at[:, cols_of(i, tn)], stage_sem.at[slot])

    def wo_copy(r, side):
        return pltpu.make_async_copy(wo_ref.at[cols_of(flip(me, r), wo_ring.shape[1]), pl.ds(side * wo_ring.shape[2], wo_ring.shape[2])],
                                     wo_ring.at[side], wo_sem.at[side])

    for side in range(2):
        wo_copy(0, side).start()

    def cv_tile(i):
        slot = ring.wait(0, i)
        s = lax.rem(i, 2)

        @pl.when(i == 0)
        def _():
            ctx_copy.wait()

        @pl.when(i >= 2)
        def _():
            stage_copy(i, s).wait()

        stage_ref[s] = dot(ctx_ref[...], ring_ref[slot]).astype(BF16)
        stage_copy(i, s).start()
        ring.refill(0, i)

    def send_output(b):
        r, h = b // n_heads, lax.rem(b, n_heads)

        @pl.when(r > 0)
        def _():
            o_remote(r, h).start()

    def step(i, now, before):
        s_now, mx_now = now
        cur = jnp.minimum(i, blocks - 1)
        r, h = cur // n_heads, lax.rem(cur, n_heads)

        @pl.when(i < n_heads)
        def _():
            for c in own(h):
                c.wait()
            for c in pair(h):
                c.wait_recv()

        @pl.when(i == 0)
        def _():
            q_local().wait()

        @pl.when((i > 0) & (i < blocks) & (h == 0))
        def _():
            q_remote(r).wait_recv()

        if before is not None:
            @pl.when(i >= 2)
            def _():
                send_output(i - 2)

            s_old, mx_old = before
            old_r, old_h = (i - 1) // n_heads, lax.rem(i - 1, n_heads)
            total = jnp.zeros((rows, 128), F32)
            acc = jnp.zeros((rows, HEAD), F32)
        q = qbuf[r, :, cols_of(h, HEAD)]
        mx = None
        for j in range(n_kb):
            s = dot_nt(q, kbuf[h, j * kb:(j + 1) * kb, :])
            s_now[:, j * kb:(j + 1) * kb] = s
            for g in range(kb // 128):
                sg = s[:, g * 128:(g + 1) * 128]
                mx = sg if mx is None else jnp.maximum(mx, sg)
            if before is not None:
                parts = []
                for g in range(kb // 128):
                    c0 = j * kb + g * 128
                    p = jnp.exp2((s_old[:, c0:c0 + 128] - mx_old[...]) * SM_C)
                    total = total + p
                    parts.append(p.astype(BF16))
                acc = acc + dot(jnp.concatenate(parts, axis=1), vbuf[old_h, j * kb:(j + 1) * kb, :])
        mx_now[...] = jnp.broadcast_to(jnp.max(mx, axis=1, keepdims=True), (rows, 128))
        if before is not None:
            qbuf[old_r, :, cols_of(old_h, HEAD)] = (acc / jnp.sum(total, axis=1, keepdims=True)).astype(BF16)

    bufs = ((s0_ref, mx0_ref), (s1_ref, mx1_ref))
    step(jnp.int32(0), bufs[0], None)

    def pair_of_steps(t, _):
        step(2 * t + 1, bufs[1], bufs[0])
        step(2 * t + 2, bufs[0], bufs[1])

        @pl.when((lax.rem(t, every) == 0) & (t < n_cv * every))
        def _():
            cv_tile(t // every)

        return 0

    every = max(1, blocks // 2 // n_cv)
    lax.fori_loop(0, blocks // 2, pair_of_steps, 0)
    send_output(jnp.int32(blocks - 1))
    for i in range(2):
        stage_copy(0, i).wait()
    width = acc_ref.shape[1]
    part = qbuf.shape[2]
    half_n = width // 2
    x_copy = pltpu.make_async_copy(x_hbm, ctx_ref.at[0:rows], ctx_sem)
    x_copy.start()
    row_ref[0] = te_ref[G1] + bm_ref[G1]
    row_ref[1] = bo_ref[...].astype(F32)

    def project(r, lhs, side, finish, ready=None):
        wo_copy(r, side).wait()
        if ready is not None:
            ready()
        for n in range(half_n // tn):
            cols = pl.ds(side * half_n + n * tn, tn)
            finish(cols, side * half_n + n * tn, dot(lhs[...], wo_ring[side, :, n * tn:(n + 1) * tn]))

    def first(cols, c0, prod):
        acc_ref[:, cols] = prod

    def middle(cols, c0, prod):
        acc_ref[:, cols] = acc_ref[:, cols] + prod

    def last(cols, c0, prod):
        total = mx0_ref[...]
        for g, p in enumerate(groups(prod)):
            k = c0 // 128 + g
            gc = slice(c0 + g * 128, c0 + (g + 1) * 128)
            x1 = ctx_ref[0:rows, gc].astype(F32) + row_ref[0, k:k + 1, :] * (acc_ref[:, gc] + p + row_ref[1, k:k + 1, :])
            acc_ref[:, gc] = x1
            total = total + x1
        mx0_ref[...] = total

    def arrived(r):
        for h in range(n_heads):
            o_remote(r, h).wait_recv()

    def x1_copy(side):
        cols = pl.ds(side * half_n, half_n)
        return pltpu.make_async_copy(acc_ref.at[:, cols], x1_out.at[:, cols], stage_sem.at[side])

    for side in range(2):
        project(0, qbuf.at[0], side, first)
        wo_copy(1, side).start()

    def chunk(r, _):
        arrived(r)
        for side in range(2):
            project(r, obuf.at[r], side, middle)
            wo_copy(r + 1, side).start()
        return 0

    lax.fori_loop(1, CHIPS - 1, chunk, 0)
    x_copy.wait()
    arrived(CHIPS - 1)
    mx0_ref[...] = jnp.zeros_like(mx0_ref)
    project(CHIPS - 1, obuf.at[CHIPS - 1], 0, last)
    project(CHIPS - 1, obuf.at[CHIPS - 1], 1, last, lambda: x1_copy(0).start())
    for h in range(n_heads):
        for c in pair(h):
            c.wait_send()

    def drain(r, _):
        q_remote(r).wait_send()
        for h in range(n_heads):
            o_remote(r, h).wait_send()
        return 0

    lax.fori_loop(1, CHIPS, drain, 0)
    x1_copy(1).start()
    sum_copy = pltpu.make_async_copy(mx0_ref, sum_out, x_sem)
    sum_copy.start()
    for side in range(2):
        x1_copy(side).wait()
    sum_copy.wait()


def attend_call(te, bm, bo, q, k, v, ctx, cwv, x, wo, cv_cols, tn):
    _, rows, part = q.shape
    half = k.shape[0]
    n_heads = part // HEAD
    text, width = ctx.shape
    flops = 8 * half * half * part + 2 * width * (text * cv_cols + rows * width)
    return pl.pallas_call(
        attend_kernel,
        out_shape=(jax.ShapeDtypeStruct((rows, width), F32), jax.ShapeDtypeStruct((rows, 128), F32), jax.ShapeDtypeStruct((text, cv_cols), BF16)),
        in_specs=[vmem_spec()] * 3 + [any_spec()] * 7,
        out_specs=[any_spec()] * 3,
        scratch_shapes=[
            pltpu.VMEM((n_heads, 2 * half, HEAD), BF16),
            pltpu.VMEM((n_heads, 2 * half, HEAD), BF16),
            pltpu.VMEM((CHIPS, rows, part), BF16),
            pltpu.VMEM((CHIPS, rows, part), BF16),
            pltpu.VMEM((rows, 2 * half), F32),
            pltpu.VMEM((rows, 2 * half), F32),
            pltpu.VMEM((rows, 128), F32),
            pltpu.VMEM((rows, 128), F32),
            pltpu.VMEM((text, width), BF16),
            pltpu.VMEM((2, text, tn), BF16),
            pltpu.VMEM((2, width, tn), BF16),
            pltpu.VMEM((rows, width), F32),
            pltpu.VMEM((2, part, width // 2), BF16),
            pltpu.VMEM((2, width // 128, 128), F32),
            pltpu.SemaphoreType.DMA((2, n_heads)),
            pltpu.SemaphoreType.DMA((2, n_heads)),
            pltpu.SemaphoreType.DMA((2, n_heads)),
            pltpu.SemaphoreType.DMA((CHIPS,)),
            pltpu.SemaphoreType.DMA((CHIPS,)),
            pltpu.SemaphoreType.DMA((CHIPS, n_heads)),
            pltpu.SemaphoreType.DMA((CHIPS, n_heads)),
            pltpu.SemaphoreType.DMA,
            pltpu.SemaphoreType.DMA((2,)),
            pltpu.SemaphoreType.DMA((2,)),
            pltpu.SemaphoreType.DMA((2,)),
            pltpu.SemaphoreType.DMA,
        ],
        compiler_params=pltpu.CompilerParams(vmem_limit_bytes=VMEM_LIMIT, collective_id=1, has_side_effects=True),
        cost_estimate=pl.CostEstimate(flops=flops, bytes_accessed=8 * half * part + 4 * width * width, transcendentals=2 * half * half * n_heads),
        name='attend',
    )(te, bm, bo, q, k, v, ctx, cwv, x, wo)


class Slabs:
    def __init__(self, slots, sems, phases):
        self.slots, self.sems, self.phases = slots, sems, phases
        self.depth, self.rows = slots.shape[0], slots.shape[1]
        self.base = [sum(p[0] for p in phases[:i]) for i in range(len(phases) + 1)]

    def copies(self, phase, i):
        n, w_ref, n_k, n_cols = self.phases[phase]
        slot = lax.rem(self.base[phase] + i, self.depth)
        cols = cols_of(i // n_k, n_cols)
        quarter = self.rows // 4
        return [pltpu.make_async_copy(w_ref.at[cols_of(lax.rem(i, n_k) * 4 + c, quarter), cols],
                                      self.slots.at[slot, pl.ds(c * quarter, quarter), pl.ds(0, n_cols)], self.sems.at[slot]) for c in range(4)]

    def start(self, phase, i):
        for c in self.copies(phase, i):
            c.start()

    def prime(self):
        for i in range(self.depth):
            self.start(0, i)

    def add_product(self, phase, i, m, lhs, k, acc_ref, fresh=False, finish=None):
        n, _, _, n_cols = self.phases[phase]
        for j in range(m):
            for c in self.copies(phase, i + j):
                c.wait()
        slots = [lax.rem(self.base[phase] + i + j, self.depth) for j in range(m)]
        per = self.rows // 128
        left = [jnp.concatenate([lhs[(k + j) * per + g] for g in range(per)], axis=1) for j in range(m)]
        c0 = 0
        waiting = None
        while c0 < n_cols:
            cols = slice(c0, min(c0 + 512, n_cols))
            total = dot(left[0], self.slots[slots[0], :, cols])
            for j in range(1, m):
                total = total + dot(left[j], self.slots[slots[j], :, cols])
            old = acc_ref[:, cols]
            acc_ref[:, cols] = total + (jnp.where(k > 0, old, 0.0) if fresh else old)
            if finish is not None:
                if waiting is not None:
                    finish(waiting)
                waiting = cols
            c0 += 512
        if waiting is not None:
            finish(waiting)
        for j in range(m):
            ahead = i + j + self.depth

            @pl.when(ahead < n)
            def _():
                self.start(phase, ahead)

            if phase + 1 < len(self.phases):
                @pl.when(ahead >= n)
                def _():
                    self.start(phase + 1, ahead - n)


def tail_kernel(te_ref, bm_ref, nw_ref, nb_ref, cgq_ref, x1_ref, sum_ref, ck_ref, cva_ref, cvb_ref, cwq_ref, cwo_ref, w1_ref, w2_ref,
                out_ref, a_ref, b_ref, xf_ref, h_ref, u_ref, ss_ref, mean_ref, vec_ref, mod_ref, kbuf, vbuf,
                s0_ref, s1_ref, s2_ref, s3_ref, stage_ref, slab_ref, slab_sem, in_sem, sum_sem, kv_sem, stage_sem):
    rows, width = xf_ref.shape
    ff = u_ref.shape[0] * 128
    text = kbuf.shape[1]
    tn = slab_ref.shape[1]
    per = tn // 128
    nt = width // tn
    n_k2 = ff // tn
    blocks = -(-ff // width)
    bc = ff // blocks
    slabs = Slabs(slab_ref, slab_sem, [
        (nt, cwq_ref, nt, width), (nt, cwo_ref, nt, width), (nt * blocks, w1_ref, nt, bc), (n_k2, w2_ref, n_k2, width)])
    x1_copy = pltpu.make_async_copy(x1_ref, xf_ref, in_sem)
    x1_copy.start()
    sum_copy = pltpu.make_async_copy(sum_ref, ss_ref, sum_sem)
    sum_copy.start()
    slabs.prime()
    load_vectors(vec_ref, (nw_ref, nb_ref, cgq_ref))
    NW, NB, CGQ = range(3)
    mod_ref[...] = te_ref[...] + bm_ref[...]

    def vec(n, k):
        return vec_ref[n, pl.ds(k, 1), :]

    def mod(n, k):
        return mod_ref[n, pl.ds(k, 1), :]

    x1_copy.wait()
    sum_copy.wait()

    def norm_to(dst, mul, add, have_sum):
        def store(k, val):
            dst[k] = val.astype(BF16)

        layer_norm(lambda k: xf_ref[:, cols_of(k, 128)], store, mul, add, rows, width, ss_ref, mean_ref, have_sum)

    norm_to(b_ref, lambda k: vec(NW, k), lambda k: vec(NB, k), True)

    def cq_slab(i, _):
        slabs.add_product(0, i, 1, b_ref, i, h_ref, True)
        return 0

    lax.fori_loop(0, nt, cq_slab, 0)
    gw = kbuf.shape[2]
    n_groups = width // gw
    heads = gw // HEAD
    n_cva = cva_ref.shape[1] // gw

    def kv_loads(g, slot):
        return (pltpu.make_async_copy(ck_ref.at[:, cols_of(g, gw)], kbuf.at[slot], kv_sem.at[0, slot]),
                pltpu.make_async_copy(cva_ref.at[:, cols_of(jnp.minimum(g, n_cva - 1), gw)], vbuf.at[slot], kv_sem.at[1, slot]),
                pltpu.make_async_copy(cvb_ref.at[:, cols_of(jnp.maximum(g - n_cva, 0), gw)], vbuf.at[slot], kv_sem.at[1, slot]))

    def kv_start(g, slot):
        k_copy, va_copy, vb_copy = kv_loads(g, slot)
        k_copy.start()

        @pl.when(g < n_cva)
        def _():
            va_copy.start()

        @pl.when(g >= n_cva)
        def _():
            vb_copy.start()

    kv_start(jnp.int32(0), jnp.int32(0))
    ss_ref[...] = jnp.zeros_like(ss_ref)

    def cq_squares(i, _):
        add_lanes(ss_ref, rows, h_ref[:, cols_of(i, tn)], True)
        return 0

    lax.fori_loop(0, nt, cq_squares, 0)
    rms_scale(ss_ref, rows, width)

    def cq_head(i, _):
        for g in range(per):
            k = i * per + g
            a_ref[k] = ((h_ref[:, cols_of(k, 128)] * ss_ref[...]) * vec(CGQ, k)).astype(BF16)
        return 0

    lax.fori_loop(0, nt, cq_head, 0)
    s_refs = (s0_ref, s1_ref, s2_ref, s3_ref)

    def cross_group(g, _):
        slot = lax.rem(g, 2)
        k_copy, v_copy, _ = kv_loads(g, slot)
        k_copy.wait()
        v_copy.wait()

        @pl.when(g + 1 < n_groups)
        def _():
            kv_start(g + 1, 1 - slot)

        tops = []

        def score(j):
            s = dot_nt(a_ref[g * heads + j], kbuf[slot, :, j * HEAD:(j + 1) * HEAD])
            s_refs[j % 4][...] = s
            parts = groups(s)
            mx = parts[0]
            for p in parts[1:]:
                mx = jnp.maximum(mx, p)
            tops.append(jnp.broadcast_to(jnp.max(mx, axis=1, keepdims=True), (rows, 128)))

        def weigh(j):
            total = jnp.zeros((rows, 128), F32)
            parts = []
            for c in range(text // 128):
                p = jnp.exp2((s_refs[j % 4][:, c * 128:(c + 1) * 128] - tops[j]) * SM_C)
                total = total + p
                parts.append(p.astype(BF16))
            acc = dot(jnp.concatenate(parts, axis=1), vbuf[slot, :, j * HEAD:(j + 1) * HEAD])
            b_ref[g * heads + j] = (acc / jnp.sum(total, axis=1, keepdims=True)).astype(BF16)

        score(0)
        for j in range(1, heads):
            score(j)
            weigh(j - 1)
        weigh(heads - 1)
        return 0

    lax.fori_loop(0, n_groups, cross_group, 0)

    def co_slab(i, _):
        slabs.add_product(1, i, 1, b_ref, i, xf_ref)
        return 0

    lax.fori_loop(0, nt, co_slab, 0)
    norm_to(a_ref, lambda k: 1.0 + mod(SC2, k), lambda k: mod(SH2, k), False)

    def f1_block(c, _):
        def f1_pair(t, _):
            slabs.add_product(2, c * nt + 2 * t, 2, a_ref, 2 * t, h_ref, True)
            return 0

        lax.fori_loop(0, nt // 2 - 1, f1_pair, 0)

        def gelu(cols):
            for g, x in enumerate(groups(h_ref[:, cols])):
                u_ref[c * (bc // 128) + cols.start // 128 + g] = gelu_tanh(x).astype(BF16)

        slabs.add_product(2, c * nt + nt - 2, 2, a_ref, nt - 2, h_ref, False, gelu)
        return 0

    lax.fori_loop(0, blocks, f1_block, 0)

    def f2_pair(t, _):
        slabs.add_product(3, 2 * t, 2, u_ref, 2 * t, h_ref, True)
        return 0

    lax.fori_loop(0, n_k2 // 2, f2_pair, 0)
    if n_k2 % 2:
        slabs.add_product(3, n_k2 - 1, 1, u_ref, n_k2 - 1, h_ref)

    def stage_copy(i, slot):
        return pltpu.make_async_copy(stage_ref.at[slot], out_ref.at[:, cols_of(i, tn)], stage_sem.at[slot])

    def finish(i, _):
        s = lax.rem(i, 2)

        @pl.when(i >= 2)
        def _():
            stage_copy(i, s).wait()

        for g in range(per):
            k = i * per + g
            stage_ref[s, :, g * 128:(g + 1) * 128] = (xf_ref[:, cols_of(k, 128)] + mod(G2, k) * h_ref[:, cols_of(k, 128)]).astype(BF16)
        stage_copy(i, s).start()
        return 0

    lax.fori_loop(0, nt, finish, 0)
    for i in range(2):
        stage_copy(0, i).wait()


def tail_call(te, bm, vectors, x1, sums, ck, cva, cvb, cwq, cwo, w1, w2, tn):
    rows, width = x1.shape
    text = ck.shape[0]
    ff = w1.shape[1]
    depth = 5
    flops = 2 * rows * width * (2 * width + 2 * ff) + 4 * rows * text * width
    return pl.pallas_call(
        tail_kernel,
        out_shape=jax.ShapeDtypeStruct((rows, width), BF16),
        in_specs=[vmem_spec()] * (2 + len(vectors)) + [any_spec()] * 9,
        out_specs=any_spec(),
        scratch_shapes=[
            pltpu.VMEM((width // 128, rows, 128), BF16),
            pltpu.VMEM((width // 128, rows, 128), BF16),
            pltpu.VMEM((rows, width), F32),
            pltpu.VMEM((rows, width), F32),
            pltpu.VMEM((ff // 128, rows, 128), BF16),
            pltpu.VMEM((rows, 128), F32),
            pltpu.VMEM((rows, 128), F32),
            pltpu.VMEM((len(vectors), width // 128, 128), F32),
            pltpu.VMEM(te.shape, F32),
            pltpu.VMEM((2, text, 8 * HEAD), BF16),
            pltpu.VMEM((2, text, 8 * HEAD), BF16),
            pltpu.VMEM((rows, text), F32),
            pltpu.VMEM((rows, text), F32),
            pltpu.VMEM((rows, text), F32),
            pltpu.VMEM((rows, text), F32),
            pltpu.VMEM((2, rows, tn), BF16),
            pltpu.VMEM((depth, tn, width), BF16),
            pltpu.SemaphoreType.DMA((depth,)),
            pltpu.SemaphoreType.DMA,
            pltpu.SemaphoreType.DMA,
            pltpu.SemaphoreType.DMA((2, 2)),
            pltpu.SemaphoreType.DMA((2,)),
        ],
        compiler_params=pltpu.CompilerParams(vmem_limit_bytes=VMEM_LIMIT),
        cost_estimate=pl.CostEstimate(flops=flops, bytes_accessed=2 * width * (2 * width + 2 * ff), transcendentals=rows * ff),
        name='tail',
    )(te, bm, *vectors, x1, sums, ck, cva, cvb, cwq, cwo, w1, w2)


def solution(mesh):
    tok_spec = P('dp', ('sp', 'uly'), None)
    batch_spec = P('dp', None, None)

    def local_block(tokens, rope_ang, t_emb, block_mod, context, attn_wq, attn_bq, attn_wk, attn_bk, attn_wv, attn_bv, attn_gq, attn_gk, attn_wo, attn_bo, norm3_w, norm3_b, cross_wq, cross_wk, cross_wv, cross_gq, cross_gk, cross_wo, ffn_w1, ffn_w2):
        x, ctx = tokens[0], context[0]
        te, bm = (m.reshape(6, -1, 128) for m in (t_emb, block_mod))
        tn = min(512, x.shape[1] // CHIPS)

        def lanes(*vectors):
            return tuple(v.reshape(-1, 128) for v in vectors)

        cv_a = max(1024, x.shape[1] * 2 // 5 // 1024 * 1024)
        cv_b = x.shape[1] - cv_a
        q, k, v, ck, cva = qkv_call(x, te, bm, rope_ang.T, lanes(attn_bq, attn_bk, attn_bv, attn_gq, attn_gk, cross_gk), ctx,
                                    attn_wv, attn_wk, attn_wq, cross_wk, cross_wv, cv_a, tn)
        x1, sums, cvb = attend_call(te, bm, *lanes(attn_bo), q, k, v, ctx, cross_wv, x, attn_wo, cv_b, tn)
        out = tail_call(te, bm, lanes(norm3_w, norm3_b, cross_gq), x1, sums, ck, cva, cvb, cross_wq, cross_wo, ffn_w1, ffn_w2, tn)
        return out[None]

    in_specs = (tok_spec, P(('sp', 'uly'), None), batch_spec, P(), batch_spec) + (P(),) * 20
    return jax.shard_map(local_block, mesh=mesh, in_specs=in_specs, out_specs=tok_spec, check_vma=False)
```
